16 devices in a mesh: dp: 2 (over y, z), tp: 8 (over x, core).
Axes of the slice: x: 4, y: 2, z: 1, core: 2. Of those that a mesh axis runs over, the one named last changes fastest.
The devices are a block of a 4x4x8 slice.
Arguments:
- x: bfloat16 [4096, 1024], P('dp'), parts along dimension 0
- gain: bfloat16 [1024], replicated
- wq: bfloat16 [1024, 16384], P(None, 'tp')
- wk: bfloat16 [1024, 16384], P(None, 'tp')
- wv: bfloat16 [1024, 16384], P(None, 'tp')
- wo: bfloat16 [16384, 1024], P('tp')
Outputs:
- output: bfloat16 [4096, 1024], P('dp'), parts along dimension 0
There are 2 independent parts. The reference program is written for one: setup_inputs(seed, part) draws one part's arguments, and reference() takes and returns one part's arrays. A program takes and returns all parts, laid end to end along the dimension named above; an argument that names none is the same for every part.
All inputs are finite; a program needn't handle non-finite values.
Results may differ from the reference program's by a relative error of at most 0.012.
Values are sent between devices in bfloat16 or wider.
A program may use at most 768 MiB of HBM per device.

```python
import jax
import jax.numpy as jnp
from jax import lax

ROWS = 2048
D = 1024
HEADS = 128
KV_HEADS = 128
HEAD = 128
THETA = 10000


def setup_inputs(seed: int = 0, part: int = 0) -> dict:
    kx, kn, kq, kk, kv, ko = jax.random.split(jax.random.key(seed), 6)

    def weights(key, rows, columns):
        return jax.random.normal(key, (rows, columns), jnp.float32) * rows**-0.5

    drawn = {
        "x": jax.random.normal(jax.random.fold_in(kx, part), (ROWS, D), jnp.float32),
        "gain": 1 + 0.1 * jax.random.normal(kn, (D,), jnp.float32),
        "wq": 2 * weights(kq, D, HEADS * HEAD),
        "wk": 2 * weights(kk, D, KV_HEADS * HEAD),
        "wv": 4 * weights(kv, D, KV_HEADS * HEAD),
        "wo": weights(ko, HEADS * HEAD, D),
    }
    return {k: v.astype(jnp.bfloat16) for k, v in drawn.items()}


def normed(x, gain):
    wide = x.astype(jnp.float32)
    scale = lax.rsqrt(jnp.mean(wide * wide, -1, keepdims=True) + 1e-6)
    return (wide * scale * gain.astype(jnp.float32)).astype(jnp.bfloat16)


def turned(t, place, theta):
    half = t.shape[-1] // 2
    angle = place.astype(jnp.float32)[:, None] * theta ** (-jnp.arange(half, dtype=jnp.float32) / half)
    cos, sin = jnp.cos(angle)[:, None], jnp.sin(angle)[:, None]
    a, b = t[..., :half].astype(jnp.float32), t[..., half:].astype(jnp.float32)
    return jnp.concatenate([a * cos - b * sin, b * cos + a * sin], -1).astype(jnp.bfloat16)


def matmul(a, w):
    return jnp.dot(a, w, preferred_element_type=jnp.float32).astype(jnp.bfloat16)


def einsum(form, a, b):
    return jnp.einsum(form, a.astype(jnp.float32), b.astype(jnp.float32))


def attention(q, k, v):
    scores = einsum("tgsd,ugd->gstu", q, k) * q.shape[-1] ** -0.5
    token = jnp.arange(q.shape[0])
    scores = jnp.where(token[:, None] >= token, scores, -jnp.inf)
    weights = jax.nn.softmax(scores, -1).astype(jnp.bfloat16)
    return einsum("gstu,ugd->tgsd", weights, v).astype(jnp.bfloat16)


def reference(x, gain, wq, wk, wv, wo):
    a, place = normed(x, gain), jnp.arange(ROWS)
    q = turned(matmul(a, wq).reshape(ROWS, HEADS, HEAD), place, THETA).reshape(ROWS, KV_HEADS, -1, HEAD)
    k = turned(matmul(a, wk).reshape(ROWS, KV_HEADS, HEAD), place, THETA)
    v = matmul(a, wv).reshape(ROWS, KV_HEADS, HEAD)
    seen = attention(q, k, v).reshape(ROWS, HEADS * HEAD)
    return (x.astype(jnp.float32) + jnp.dot(seen, wo, preferred_element_type=jnp.float32)).astype(jnp.bfloat16)
```

```python
import functools

import jax
import jax.numpy as jnp
import numpy as np
from jax import lax
from jax.experimental import pallas as pl
from jax.experimental.pallas import tpu as pltpu
from jax.sharding import PartitionSpec as P

HEAD = 128
THETA = 10000
HIDDEN = -2e30
LOG2E = 1.4426950408889634
VMEM = 60 * 2**20
COLS = 512
ROWS = 512
BQ = 256


def dot(a, b):
    return lax.dot_general(a, b, (((1,), (0,)), ((), ())), preferred_element_type=jnp.float32)


def table(rows):
    half = HEAD // 2
    angle = np.arange(rows, dtype=np.float32)[:, None] * (np.float32(THETA) ** (-np.arange(half, dtype=np.float32) / half)).astype(np.float32)
    return np.concatenate([np.cos(angle.astype(np.float64)), np.sin(angle.astype(np.float64))], -1).astype(np.float32)


def project_kernel(x_ref, gain_ref, cs_ref, wq_ref, wk_ref, wv_ref, qt_ref, k_ref, vt_ref, some_s, cos_s, sin_s, flat_s, tall_s, sems):
    n = pl.program_id(0)
    rows = some_s.shape[0]
    per = pl.num_programs(0) // 3
    slot = lax.rem(n, 2)
    pieces = [pl.ds(at, ROWS) for at in range(0, rows, ROWS)]

    @pl.when(n == 0)
    def _():
        gain = gain_ref[...].astype(jnp.float32)
        low = lax.broadcasted_iota(jnp.int32, (ROWS // 4, HEAD), 1) < HEAD // 2

        def prepare(i, _):
            here = pl.ds(i * (ROWS // 4), ROWS // 4)
            wide = x_ref[here, :].astype(jnp.float32)
            scale = lax.rsqrt(jnp.mean(wide * wide, -1, keepdims=True) + 1e-6)
            some_s[here, :] = (wide * scale * gain).astype(jnp.bfloat16)
            cs = cs_ref[here, :]
            other = pltpu.roll(cs, HEAD // 2, 1)
            cos_s[here, :] = jnp.where(low, cs, other)
            sin_s[here, :] = jnp.where(low, -other, cs)

        lax.fori_loop(0, rows // (ROWS // 4), prepare, None)

    def turned(t, here):
        t = t.astype(jnp.bfloat16).astype(jnp.float32)
        return (t * cos_s[here, :] + pltpu.roll(t, HEAD // 2, 1) * sin_s[here, :]).astype(jnp.bfloat16)

    def flat_out(i, s, ref):
        return pltpu.make_async_copy(flat_s.at[s], ref.at[pl.ds(pl.multiple_of(i * COLS, COLS), COLS), :], sems.at[s])

    def tall_out(i, s):
        return pltpu.make_async_copy(tall_s.at[s], k_ref.at[:, pl.ds(pl.multiple_of(i * COLS, COLS), COLS)], sems.at[s])

    @pl.when((n >= 2) & (n < per + 2))
    def _():
        flat_out(n - 2, slot, qt_ref).wait()

    @pl.when((n >= per + 2) & (n < 2 * per + 2))
    def _():
        tall_out(n - 2 - per, slot).wait()

    @pl.when(n >= 2 * per + 2)
    def _():
        flat_out(n - 2 - 2 * per, slot, vt_ref).wait()

    @pl.when(n < per)
    def _():
        for here in pieces:
            t = dot(some_s[here, :], wq_ref[...])
            for c in range(0, COLS, HEAD):
                flat_s[slot, c : c + HEAD, here] = turned(t[:, c : c + HEAD], here).T
        flat_out(n, slot, qt_ref).start()

    @pl.when((n >= per) & (n < 2 * per))
    def _():
        for here in pieces:
            t = dot(some_s[here, :], wk_ref[...])
            for c in range(0, COLS, HEAD):
                tall_s[slot, here, c : c + HEAD] = turned(t[:, c : c + HEAD], here)
        tall_out(n - per, slot).start()

    @pl.when(n >= 2 * per)
    def _():
        for here in pieces:
            t = dot(some_s[here, :], wv_ref[...]).astype(jnp.bfloat16)
            for c in range(0, COLS, HEAD):
                flat_s[slot, c : c + HEAD, here] = t[:, c : c + HEAD].T
        flat_out(n - 2 * per, slot, vt_ref).start()

    @pl.when(n == 3 * per - 1)
    def _():
        flat_out(n - 1 - 2 * per, 1 - slot, vt_ref).wait()
        flat_out(n - 2 * per, slot, vt_ref).wait()


def project(x, gain, wq, wk, wv):
    rows, wide = x.shape
    columns = wq.shape[1]
    per = columns // COLS
    whole = lambda n: (0, 0)
    one = pl.Buffered(buffer_count=1)
    weight = lambda k: pl.BlockSpec((wide, COLS), lambda n: (0, jnp.clip(n - k * per, 0, per - 1)))
    any_ = pl.BlockSpec(memory_space=pl.ANY)
    return pl.pallas_call(
        project_kernel,
        grid=(3 * per,),
        in_specs=[
            pl.BlockSpec((rows, wide), whole, pipeline_mode=one),
            pl.BlockSpec((1, wide), whole, pipeline_mode=one),
            pl.BlockSpec((rows, HEAD), whole, pipeline_mode=one),
            weight(0), weight(1), weight(2),
        ],
        out_specs=[any_, any_, any_],
        out_shape=[
            jax.ShapeDtypeStruct((columns, rows), jnp.bfloat16),
            jax.ShapeDtypeStruct((rows, columns), jnp.bfloat16),
            jax.ShapeDtypeStruct((columns, rows), jnp.bfloat16),
        ],
        scratch_shapes=[
            pltpu.VMEM((rows, wide), jnp.bfloat16),
            pltpu.VMEM((rows, HEAD), jnp.float32),
            pltpu.VMEM((rows, HEAD), jnp.float32),
            pltpu.VMEM((2, COLS, rows), jnp.bfloat16),
            pltpu.VMEM((2, rows, COLS), jnp.bfloat16),
            pltpu.SemaphoreType.DMA((2,)),
        ],
        compiler_params=pltpu.CompilerParams(dimension_semantics=("arbitrary",), vmem_limit_bytes=VMEM),
        cost_estimate=pl.CostEstimate(flops=6 * rows * wide * columns, transcendentals=0, bytes_accessed=6 * wide * columns + 6 * rows * columns),
    )(x, gain.reshape(1, -1), jnp.asarray(table(rows)), wq, wk, wv)


def attend_kernel(qt_ref, k_ref, vt_ref, wo_ref, out_ref, q_s, k_s, v_s, wo_s, sa, sb, seen_s, term_s, sems, wo_sem, out_sems):
    rows, columns = k_s.shape
    heads = columns // HEAD
    blocks = rows // BQ
    e = HEAD**-0.5 * LOG2E
    scores = (sa, sb)

    def fetch(i):
        here = pl.ds(i * BQ, BQ)
        return (
            pltpu.make_async_copy(qt_ref.at[:, here], q_s.at[:, here], sems.at[i, 0]),
            pltpu.make_async_copy(k_ref.at[here, :], k_s.at[here, :], sems.at[i, 1]),
            pltpu.make_async_copy(vt_ref.at[:, here], v_s.at[:, here], sems.at[i, 2]),
        )

    get_wo = pltpu.make_async_copy(wo_ref, wo_s, wo_sem)
    for i in range(blocks):
        for copy in fetch(i):
            copy.start()
        if i == 0:
            get_wo.start()

    ones = jnp.ones((16, BQ), jnp.bfloat16)

    def column(h):
        return pl.ds(pl.multiple_of(h * HEAD, HEAD), HEAD)

    for iq in range(blocks):
        here = pl.ds(iq * BQ, BQ)
        for copy in fetch(iq):
            copy.wait()
        tiles = iq + 1
        unroll = max(4, min(heads, 16 // tiles))
        unroll = max(u for u in (16, 8, 4, 2) if u <= unroll and heads % u == 0)

        def first(h, s_ref, j):
            tile = pl.ds(j * BQ, BQ)
            s = dot(k_s[tile, column(h)], q_s[column(h), here])
            if j == iq:
                seen = lax.broadcasted_iota(jnp.int32, (BQ, BQ), 0) <= lax.broadcasted_iota(jnp.int32, (BQ, BQ), 1)
                s = jnp.where(seen, s, HIDDEN)
            s_ref[tile, :] = s
            return s.reshape(BQ // 8, 8, BQ).max(0)

        def second(h, s_ref, j, top):
            tile = pl.ds(j * BQ, BQ)
            p = jnp.exp2((s_ref[tile, :] - top) * e).astype(jnp.bfloat16)
            return dot(jnp.concatenate([v_s[column(h), tile], ones], 0), p)

        def peak(parts):
            m = parts[0]
            for part in parts[1:]:
                m = jnp.maximum(m, part)
            return m.max(axis=0, keepdims=True)

        def finish(h, total):
            seen_s[:, column(h)] = (total[:HEAD] * (1 / total[HEAD : HEAD + 1])).astype(jnp.bfloat16).T

        def group(g, top):
            for u in range(unroll):
                h = g * unroll + u
                later = jnp.minimum(h + 1, heads - 1)
                parts, total = [], None
                for j in range(tiles):
                    parts.append(first(later, scores[(u + 1) % 2], j))
                    got = second(h, scores[u % 2], j, top)
                    total = got if total is None else total + got
                finish(h, total)
                top = peak(parts)
            return top

        top = peak([first(0, scores[0], j) for j in range(tiles)])
        lax.fori_loop(0, heads // unroll, group, top)
        if iq == 0:
            get_wo.wait()
        term_s[here, :] = dot(seen_s[...], wo_s[...]).astype(jnp.bfloat16)
        pltpu.make_async_copy(term_s.at[here, :], out_ref.at[here, :], out_sems.at[iq]).start()

    for iq in range(blocks):
        here = pl.ds(iq * BQ, BQ)
        pltpu.make_async_copy(term_s.at[here, :], out_ref.at[here, :], out_sems.at[iq]).wait()


def attend(qt, k, vt, wo):
    rows, columns = k.shape
    wide = wo.shape[1]
    any_ = pl.BlockSpec(memory_space=pl.ANY)
    bf16 = jnp.bfloat16
    return pl.pallas_call(
        attend_kernel,
        in_specs=[any_] * 4,
        out_specs=any_,
        out_shape=jax.ShapeDtypeStruct((rows, wide), bf16),
        scratch_shapes=[
            pltpu.VMEM((columns, rows), bf16),
            pltpu.VMEM((rows, columns), bf16),
            pltpu.VMEM((columns, rows), bf16),
            pltpu.VMEM(wo.shape, bf16),
            pltpu.VMEM((rows, BQ), jnp.float32),
            pltpu.VMEM((rows, BQ), jnp.float32),
            pltpu.VMEM((BQ, columns), bf16),
            pltpu.VMEM((rows, wide), bf16),
            pltpu.SemaphoreType.DMA((rows // BQ, 3)),
            pltpu.SemaphoreType.DMA,
            pltpu.SemaphoreType.DMA((rows // BQ,)),
        ],
        compiler_params=pltpu.CompilerParams(vmem_limit_bytes=VMEM),
        cost_estimate=pl.CostEstimate(flops=2 * rows * rows * columns + 2 * rows * wide * columns, transcendentals=rows * rows * columns // HEAD // 2, bytes_accessed=8 * rows * columns),
    )(qt, k, vt, wo)


def solution(mesh):
    def step(x, gain, wq, wk, wv, wo):
        qt, k, vt = project(x, gain, wq, wk, wv)
        term = attend(qt, k, vt, wo)
        y = lax.psum(term, "tp")
        return (x.astype(jnp.float32) + y.astype(jnp.float32)).astype(jnp.bfloat16)

    tokens, columns = P("dp", None), P(None, "tp")
    return jax.shard_map(
        step,
        mesh=mesh,
        in_specs=(tokens, P(None), columns, columns, columns, P("tp", None)),
        out_specs=tokens,
        check_vma=False,
    )
```

```python
import functools

import jax
import jax.numpy as jnp
import numpy as np
from jax import lax
from jax.experimental import pallas as pl
from jax.experimental.pallas import tpu as pltpu
from jax.sharding import PartitionSpec as P

HEAD = 128
THETA = 10000
HIDDEN = -2e30
LOG2E = 1.4426950408889634
VMEM = 60 * 2**20
COLS = 512
ROWS = 512
BQ = 256


def dot(a, b):
    return lax.dot_general(a, b, (((1,), (0,)), ((), ())), preferred_element_type=jnp.float32)


def table(rows):
    half = HEAD // 2
    angle = np.arange(rows, dtype=np.float32)[:, None] * (np.float32(THETA) ** (-np.arange(half, dtype=np.float32) / half)).astype(np.float32)
    return np.concatenate([np.cos(angle.astype(np.float64)), np.sin(angle.astype(np.float64))], -1).astype(np.float32)


def project_kernel(x_ref, gain_ref, cs_ref, wq_ref, wk_ref, wv_ref, qt_ref, k_ref, vt_ref, some_s, cos_s, sin_s, flat_s, tall_s, sems):
    n = pl.program_id(0)
    rows = some_s.shape[0]
    per = pl.num_programs(0) // 3
    slot = lax.rem(n, 2)
    pieces = [pl.ds(at, ROWS) for at in range(0, rows, ROWS)]

    @pl.when(n == 0)
    def _():
        gain = gain_ref[...].astype(jnp.float32)
        low = lax.broadcasted_iota(jnp.int32, (ROWS // 4, HEAD), 1) < HEAD // 2

        def prepare(i, _):
            here = pl.ds(i * (ROWS // 4), ROWS // 4)
            wide = x_ref[here, :].astype(jnp.float32)
            scale = lax.rsqrt(jnp.mean(wide * wide, -1, keepdims=True) + 1e-6)
            some_s[here, :] = (wide * scale * gain).astype(jnp.bfloat16)
            cs = cs_ref[here, :]
            other = pltpu.roll(cs, HEAD // 2, 1)
            cos_s[here, :] = jnp.where(low, cs, other)
            sin_s[here, :] = jnp.where(low, -other, cs)

        lax.fori_loop(0, rows // (ROWS // 4), prepare, None)

    def turned(t, here):
        t = t.astype(jnp.bfloat16).astype(jnp.float32)
        return (t * cos_s[here, :] + pltpu.roll(t, HEAD // 2, 1) * sin_s[here, :]).astype(jnp.bfloat16)

    def flat_out(i, s, ref):
        return pltpu.make_async_copy(flat_s.at[s], ref.at[pl.ds(pl.multiple_of(i * COLS, COLS), COLS), :], sems.at[s])

    def tall_out(i, s):
        return pltpu.make_async_copy(tall_s.at[s], k_ref.at[:, pl.ds(pl.multiple_of(i * COLS, COLS), COLS)], sems.at[s])

    @pl.when((n >= 2) & (n < per + 2))
    def _():
        flat_out(n - 2, slot, qt_ref).wait()

    @pl.when((n >= per + 2) & (n < 2 * per + 2))
    def _():
        tall_out(n - 2 - per, slot).wait()

    @pl.when(n >= 2 * per + 2)
    def _():
        flat_out(n - 2 - 2 * per, slot, vt_ref).wait()

    @pl.when(n < per)
    def _():
        for here in pieces:
            t = dot(some_s[here, :], wq_ref[...])
            for c in range(0, COLS, HEAD):
                flat_s[slot, c : c + HEAD, here] = turned(t[:, c : c + HEAD], here).T
        flat_out(n, slot, qt_ref).start()

    @pl.when((n >= per) & (n < 2 * per))
    def _():
        for here in pieces:
            t = dot(some_s[here, :], wk_ref[...])
            for c in range(0, COLS, HEAD):
                tall_s[slot, here, c : c + HEAD] = turned(t[:, c : c + HEAD], here)
        tall_out(n - per, slot).start()

    @pl.when(n >= 2 * per)
    def _():
        for here in pieces:
            t = dot(some_s[here, :], wv_ref[...]).astype(jnp.bfloat16)
            for c in range(0, COLS, HEAD):
                flat_s[slot, c : c + HEAD, here] = t[:, c : c + HEAD].T
        flat_out(n - 2 * per, slot, vt_ref).start()

    @pl.when(n == 3 * per - 1)
    def _():
        flat_out(n - 1 - 2 * per, 1 - slot, vt_ref).wait()
        flat_out(n - 2 * per, slot, vt_ref).wait()


def project(x, gain, wq, wk, wv):
    rows, wide = x.shape
    columns = wq.shape[1]
    per = columns // COLS
    whole = lambda n: (0, 0)
    one = pl.Buffered(buffer_count=1)
    weight = lambda k: pl.BlockSpec((wide, COLS), lambda n: (0, jnp.clip(n - k * per, 0, per - 1)))
    any_ = pl.BlockSpec(memory_space=pl.ANY)
    return pl.pallas_call(
        project_kernel,
        grid=(3 * per,),
        in_specs=[
            pl.BlockSpec((rows, wide), whole, pipeline_mode=one),
            pl.BlockSpec((1, wide), whole, pipeline_mode=one),
            pl.BlockSpec((rows, HEAD), whole, pipeline_mode=one),
            weight(0), weight(1), weight(2),
        ],
        out_specs=[any_, any_, any_],
        out_shape=[
            jax.ShapeDtypeStruct((columns, rows), jnp.bfloat16),
            jax.ShapeDtypeStruct((rows, columns), jnp.bfloat16),
            jax.ShapeDtypeStruct((columns, rows), jnp.bfloat16),
        ],
        scratch_shapes=[
            pltpu.VMEM((rows, wide), jnp.bfloat16),
            pltpu.VMEM((rows, HEAD), jnp.float32),
            pltpu.VMEM((rows, HEAD), jnp.float32),
            pltpu.VMEM((2, COLS, rows), jnp.bfloat16),
            pltpu.VMEM((2, rows, COLS), jnp.bfloat16),
            pltpu.SemaphoreType.DMA((2,)),
        ],
        compiler_params=pltpu.CompilerParams(dimension_semantics=("arbitrary",), vmem_limit_bytes=VMEM),
        cost_estimate=pl.CostEstimate(flops=6 * rows * wide * columns, transcendentals=0, bytes_accessed=6 * wide * columns + 6 * rows * columns),
    )(x, gain.reshape(1, -1), jnp.asarray(table(rows)), wq, wk, wv)


def attend_kernel(n, qt_ref, k_ref, vt_ref, wo_ref, x_ref, y_ref, q_s, k_s, v_s, wo_s, sa, sb, seen_s, sum_s, x_s, y_s,
                  give_s, take_s, far_out, far_in, near_out, near_in, sems, wo_sem, x_sems, y_sems, send_sems, recv_sems):
    rows, columns = k_s.shape
    heads = columns // HEAD
    blocks = rows // BQ
    e = HEAD**-0.5 * LOG2E
    scores = (sa, sb)
    chips = n // 2
    me = lax.axis_index("tp")
    core, chip = lax.rem(me, 2), lax.div(me, 2)
    after, before, across = (lax.rem(chip + d, chips) for d in (1, chips - 1, 2))
    right, left, partner = 2 * after + core, 2 * before + core, 2 * chip + 1 - core
    part = BQ // n
    early, late = pl.ds(0, part // 2), pl.ds(part // 2, part // 2)

    def fetch(i):
        here = pl.ds(i * BQ, BQ)
        return (
            pltpu.make_async_copy(qt_ref.at[:, here], q_s.at[:, here], sems.at[i, 0]),
            pltpu.make_async_copy(k_ref.at[here, :], k_s.at[here, :], sems.at[i, 1]),
            pltpu.make_async_copy(vt_ref.at[:, here], v_s.at[:, here], sems.at[i, 2]),
        )

    def fetch_x(i):
        return pltpu.make_async_copy(x_ref.at[i, core, chip], x_s.at[i], x_sems.at[i])

    get_wo = pltpu.make_async_copy(wo_ref, wo_s, wo_sem)
    for i in range(blocks):
        for copy in fetch(i):
            copy.start()
        if i == 0:
            get_wo.start()
    for i in range(blocks):
        fetch_x(i).start()

    barrier = pltpu.get_barrier_semaphore()
    for other in (left, right, partner):
        pl.semaphore_signal(barrier, inc=1, device_id={"tp": other}, device_id_type=pl.DeviceIdType.MESH)
    pl.semaphore_wait(barrier, 3)

    def remote(c, kind, src, dst, to):
        return pltpu.make_async_remote_copy(src, dst, send_sems.at[c, kind], recv_sems.at[c, kind], device_id={"tp": to},
                                            device_id_type=pl.DeviceIdType.MESH)

    def copies(c):
        mine, other = y_s.at[c, core], y_s.at[c, core]
        return {
            0: (give_s.at[c], take_s.at[c], partner),
            1: (far_out.at[c, 0], far_in.at[c, 0], right),
            2: (far_out.at[c, 1], far_in.at[c, 1], left),
            3: (near_out.at[c, 0], near_in.at[c, 0], right),
            4: (near_out.at[c, 1], near_in.at[c, 1], left),
            5: (mine.at[chip], other.at[chip], right),
            6: (mine.at[chip], other.at[chip], left),
            7: (mine.at[chip], other.at[chip], partner),
            8: (mine.at[before, early], other.at[before, early], right),
            9: (mine.at[after, late], other.at[after, late], left),
            10: (mine.at[before], other.at[before], partner),
            11: (mine.at[after], other.at[after], partner),
            12: (mine.at[across], other.at[across], partner),
        }

    def start(c, *kinds):
        for kind in kinds:
            remote(c, kind, *copies(c)[kind]).start()

    def arrived(c, *kinds):
        for kind in kinds:
            remote(c, kind, *copies(c)[kind]).wait_recv()

    def y_out(c):
        return pltpu.make_async_copy(y_s.at[c], y_ref.at[c], y_sems.at[c])

    f32, bf16 = jnp.float32, jnp.bfloat16

    def stage(c, s):
        if s == 0:
            start(c, 0)
        if s == 1:
            arrived(c, 0)
            for q in range(chips):
                sum_s[c, q] = sum_s[c, q] + take_s[c, q].astype(f32)
            far_out[c, 0] = sum_s[c, across, early, :].astype(bf16)
            far_out[c, 1] = sum_s[c, across, late, :].astype(bf16)
            start(c, 1, 2)
        if s == 2:
            arrived(c, 1, 2)
            near_out[c, 0, early, :] = (sum_s[c, after, early, :] + far_in[c, 0].astype(f32)).astype(bf16)
            near_out[c, 0, late, :] = sum_s[c, after, late, :].astype(bf16)
            near_out[c, 1, early, :] = sum_s[c, before, early, :].astype(bf16)
            near_out[c, 1, late, :] = (sum_s[c, before, late, :] + far_in[c, 1].astype(f32)).astype(bf16)
            start(c, 3, 4)
        if s == 3:
            arrived(c, 3, 4)
            fetch_x(c).wait()
            total = sum_s[c, chip] + near_in[c, 0].astype(f32) + near_in[c, 1].astype(f32)
            y_s[c, core, chip] = (x_s[c].astype(f32) + total).astype(bf16)
            start(c, 5, 6, 7)
        if s == 4:
            arrived(c, 5, 6, 7)
            start(c, 8, 9, 10, 11)
        if s == 5:
            arrived(c, 8, 9, 10, 11)
            start(c, 12)
        if s == 6:
            arrived(c, 12)
            y_out(c).start()

    last_stage = 6
    flight = []

    def due():
        now = [(c, s) for c, s in flight]
        flight[:] = [(c, s + 1) for c, s in flight if s < last_stage]
        return now

    def run(now):
        for c, s in now:
            stage(c, s)

    ones = jnp.ones((16, BQ), bf16)
    half = BQ // 2
    my_rows, other_rows = pl.multiple_of(core * half, half), pl.multiple_of((1 - core) * half, half)

    def column(h):
        return pl.ds(pl.multiple_of(h * HEAD, HEAD), HEAD)

    for iq in range(blocks):
        here = pl.ds(iq * BQ, BQ)
        for copy in fetch(iq):
            copy.wait()
        tiles = iq + 1
        unroll = max(4, min(heads, 16 // tiles))
        unroll = max(u for u in (16, 8, 4, 2) if u <= unroll and heads % u == 0)

        def first(h, s_ref, j):
            tile = pl.ds(j * BQ, BQ)
            s = dot(k_s[tile, column(h)], q_s[column(h), here])
            if j == iq:
                seen = lax.broadcasted_iota(jnp.int32, (BQ, BQ), 0) <= lax.broadcasted_iota(jnp.int32, (BQ, BQ), 1)
                s = jnp.where(seen, s, HIDDEN)
            s_ref[tile, :] = s
            return s.reshape(BQ // 8, 8, BQ).max(0)

        def second(h, s_ref, j, top):
            tile = pl.ds(j * BQ, BQ)
            p = jnp.exp2((s_ref[tile, :] - top) * e).astype(bf16)
            return dot(jnp.concatenate([v_s[column(h), tile], ones], 0), p)

        def peak(parts):
            m = parts[0]
            for part in parts[1:]:
                m = jnp.maximum(m, part)
            return m.max(axis=0, keepdims=True)

        def finish(h, total):
            done = (total[:HEAD] * (1 / total[HEAD : HEAD + 1])).astype(bf16).T
            seen_s[pl.ds(my_rows, half), column(h)] = done[:half]
            seen_s[pl.ds(other_rows, half), column(h)] = done[half:]

        plan = [due() for _ in range(heads // unroll)]

        def group(g, top):
            for u in range(unroll):
                h = g * unroll + u
                later = jnp.minimum(h + 1, heads - 1)
                parts, total = [], None
                for j in range(tiles):
                    parts.append(first(later, scores[(u + 1) % 2], j))
                    got = second(h, scores[u % 2], j, top)
                    total = got if total is None else total + got
                finish(h, total)
                top = peak(parts)
            for i, now in enumerate(plan):
                if now:
                    pl.when(g == i)(functools.partial(run, now))
            return top

        top = peak([first(0, scores[0], j) for j in range(tiles)])
        lax.fori_loop(0, heads // unroll, group, top)
        if iq == 0:
            get_wo.wait()
        term = dot(seen_s[...], wo_s[...])
        for q in range(chips):
            sum_s[iq, q] = term[q * part : (q + 1) * part]
            give_s[iq, q] = term[half + q * part : half + (q + 1) * part].astype(bf16)
        flight.append((iq, 0))
        run(due())

    while flight:
        run(due())
    for c in range(blocks):
        for kind, copy in copies(c).items():
            remote(c, kind, *copy).wait_send()
        y_out(c).wait()


def attend(n, qt, k, vt, wo, x):
    rows, columns = k.shape
    wide = wo.shape[1]
    any_ = pl.BlockSpec(memory_space=pl.ANY)
    bf16, f32 = jnp.bfloat16, jnp.float32
    blocks, chips, part = rows // BQ, n // 2, BQ // n
    cut = (blocks, 2, chips, part, wide)
    kinds = 13
    y = pl.pallas_call(
        functools.partial(attend_kernel, n),
        in_specs=[any_] * 5,
        out_specs=any_,
        out_shape=jax.ShapeDtypeStruct(cut, bf16),
        scratch_shapes=[
            pltpu.VMEM((columns, rows), bf16),
            pltpu.VMEM((rows, columns), bf16),
            pltpu.VMEM((columns, rows), bf16),
            pltpu.VMEM(wo.shape, bf16),
            pltpu.VMEM((rows, BQ), f32),
            pltpu.VMEM((rows, BQ), f32),
            pltpu.VMEM((BQ, columns), bf16),
            pltpu.VMEM((blocks, chips, part, wide), f32),
            pltpu.VMEM((blocks, part, wide), bf16),
            pltpu.VMEM(cut, bf16),
            pltpu.VMEM((blocks, chips, part, wide), bf16),
            pltpu.VMEM((blocks, chips, part, wide), bf16),
            pltpu.VMEM((blocks, 2, part // 2, wide), bf16),
            pltpu.VMEM((blocks, 2, part // 2, wide), bf16),
            pltpu.VMEM((blocks, 2, part, wide), bf16),
            pltpu.VMEM((blocks, 2, part, wide), bf16),
            pltpu.SemaphoreType.DMA((blocks, 3)),
            pltpu.SemaphoreType.DMA,
            pltpu.SemaphoreType.DMA((blocks,)),
            pltpu.SemaphoreType.DMA((blocks,)),
            pltpu.SemaphoreType.DMA((blocks, kinds)),
            pltpu.SemaphoreType.DMA((blocks, kinds)),
        ],
        compiler_params=pltpu.CompilerParams(vmem_limit_bytes=VMEM, collective_id=0, has_side_effects=True),
        cost_estimate=pl.CostEstimate(flops=2 * rows * rows * columns + 2 * rows * wide * columns, transcendentals=rows * rows * columns // HEAD // 2, bytes_accessed=8 * rows * columns),
    )(qt, k, vt, wo, x.reshape(cut))
    return y.reshape(rows, wide)


def solution(mesh):
    n = mesh.shape["tp"]

    def step(x, gain, wq, wk, wv, wo):
        qt, k, vt = project(x, gain, wq, wk, wv)
        return attend(n, qt, k, vt, wo, x)

    tokens, columns = P("dp", None), P(None, "tp")
    return jax.shard_map(
        step,
        mesh=mesh,
        in_specs=(tokens, P(None), columns, columns, columns, P("tp", None)),
        out_specs=tokens,
        check_vma=False,
    )
```

```python
import functools

import jax
import jax.numpy as jnp
import numpy as np
from jax import lax
from jax.experimental import pallas as pl
from jax.experimental.pallas import tpu as pltpu
from jax.sharding import PartitionSpec as P

HEAD = 128
THETA = 10000
HIDDEN = -2e30
LOG2E = 1.4426950408889634
VMEM = 60 * 2**20
COLS = 512
ROWS = 512
BQ = 256
TRAVEL = (2.2, 3.8, 4.6, 4.6, 3.8, 2.2, 0)


def dot(a, b):
    return lax.dot_general(a, b, (((1,), (0,)), ((), ())), preferred_element_type=jnp.float32)


def table(rows):
    half = HEAD // 2
    angle = np.arange(rows, dtype=np.float32)[:, None] * (np.float32(THETA) ** (-np.arange(half, dtype=np.float32) / half)).astype(np.float32)
    return np.concatenate([np.cos(angle.astype(np.float64)), np.sin(angle.astype(np.float64))], -1).astype(np.float32)


def project_kernel(x_ref, gain_ref, cs_ref, wq_ref, wk_ref, wv_ref, qt_ref, k_ref, vt_ref, some_s, cos_s, sin_s, flat_s, tall_s, sems):
    n = pl.program_id(0)
    rows = some_s.shape[0]
    per = pl.num_programs(0) // 3
    slot = lax.rem(n, 2)
    pieces = [pl.ds(at, ROWS) for at in range(0, rows, ROWS)]

    @pl.when(n == 0)
    def _():
        gain = gain_ref[...].astype(jnp.float32).reshape(1, -1)
        low = lax.broadcasted_iota(jnp.int32, (ROWS // 4, HEAD), 1) < HEAD // 2

        def prepare(i, _):
            here = pl.ds(i * (ROWS // 4), ROWS // 4)
            wide = x_ref[here, :].astype(jnp.float32)
            scale = lax.rsqrt(jnp.mean(wide * wide, -1, keepdims=True) + 1e-6)
            some_s[here, :] = (wide * scale * gain).astype(jnp.bfloat16)
            cs = cs_ref[here, :]
            other = pltpu.roll(cs, HEAD // 2, 1)
            cos_s[here, :] = jnp.where(low, cs, other)
            sin_s[here, :] = jnp.where(low, -other, cs)

        lax.fori_loop(0, rows // (ROWS // 4), prepare, None)

    def turned(t, here):
        t = t.astype(jnp.bfloat16).astype(jnp.float32)
        return (t * cos_s[here, :] + pltpu.roll(t, HEAD // 2, 1) * sin_s[here, :]).astype(jnp.bfloat16)

    def flat_out(i, s, ref):
        return pltpu.make_async_copy(flat_s.at[s], ref.at[pl.ds(pl.multiple_of(i * COLS, COLS), COLS), :], sems.at[s])

    def tall_out(i, s):
        return pltpu.make_async_copy(tall_s.at[s], k_ref.at[:, pl.ds(pl.multiple_of(i * COLS, COLS), COLS)], sems.at[s])

    @pl.when((n >= 2) & (n < per + 2))
    def _():
        flat_out(n - 2, slot, qt_ref).wait()

    @pl.when((n >= per + 2) & (n < 2 * per + 2))
    def _():
        tall_out(n - 2 - per, slot).wait()

    @pl.when(n >= 2 * per + 2)
    def _():
        flat_out(n - 2 - 2 * per, slot, vt_ref).wait()

    @pl.when(n < per)
    def _():
        for here in pieces:
            t = dot(some_s[here, :], wq_ref[...])
            for c in range(0, COLS, HEAD):
                flat_s[slot, c : c + HEAD, here] = turned(t[:, c : c + HEAD], here).T
        flat_out(n, slot, qt_ref).start()

    @pl.when((n >= per) & (n < 2 * per))
    def _():
        for here in pieces:
            t = dot(some_s[here, :], wk_ref[...])
            for c in range(0, COLS, HEAD):
                tall_s[slot, here, c : c + HEAD] = turned(t[:, c : c + HEAD], here)
        tall_out(n - per, slot).start()

    @pl.when(n >= 2 * per)
    def _():
        for here in pieces:
            t = dot(some_s[here, :], wv_ref[...]).astype(jnp.bfloat16)
            for c in range(0, COLS, HEAD):
                flat_s[slot, c : c + HEAD, here] = t[:, c : c + HEAD].T
        flat_out(n - 2 * per, slot, vt_ref).start()

    @pl.when(n == 3 * per - 1)
    def _():
        flat_out(n - 1 - 2 * per, 1 - slot, vt_ref).wait()
        flat_out(n - 2 * per, slot, vt_ref).wait()


def project(x, gain, wq, wk, wv):
    rows, wide = x.shape
    columns = wq.shape[1]
    per = columns // COLS
    whole = lambda n: (0, 0)
    one = pl.Buffered(buffer_count=1)
    weight = lambda k: pl.BlockSpec((wide, COLS), lambda n: (0, jnp.clip(n - k * per, 0, per - 1)))
    any_ = pl.BlockSpec(memory_space=pl.ANY)
    return pl.pallas_call(
        project_kernel,
        grid=(3 * per,),
        in_specs=[
            pl.BlockSpec((rows, wide), whole, pipeline_mode=one),
            pl.BlockSpec((wide,), lambda n: (0,), pipeline_mode=one),
            pl.BlockSpec((rows, HEAD), whole, pipeline_mode=one),
            weight(0), weight(1), weight(2),
        ],
        out_specs=[any_, any_, any_],
        out_shape=[
            jax.ShapeDtypeStruct((columns, rows), jnp.bfloat16),
            jax.ShapeDtypeStruct((rows, columns), jnp.bfloat16),
            jax.ShapeDtypeStruct((columns, rows), jnp.bfloat16),
        ],
        scratch_shapes=[
            pltpu.VMEM((rows, wide), jnp.bfloat16),
            pltpu.VMEM((rows, HEAD), jnp.float32),
            pltpu.VMEM((rows, HEAD), jnp.float32),
            pltpu.VMEM((2, COLS, rows), jnp.bfloat16),
            pltpu.VMEM((2, rows, COLS), jnp.bfloat16),
            pltpu.SemaphoreType.DMA((2,)),
        ],
        compiler_params=pltpu.CompilerParams(dimension_semantics=("arbitrary",), vmem_limit_bytes=VMEM),
        cost_estimate=pl.CostEstimate(flops=6 * rows * wide * columns, transcendentals=0, bytes_accessed=6 * wide * columns + 6 * rows * columns),
    )(x, gain, jnp.asarray(table(rows)), wq, wk, wv)


def attend_kernel(n, qt_ref, k_ref, vt_ref, wo_ref, x_ref, y_s, q_s, k_s, v_s, wo_s, sa, sb, seen_s, sum_s, x_s,
                  give_s, take_s, far_out, far_in, near_out, near_in, sems, wo_sem, x_sems, send_sems, recv_sems):
    rows, columns = k_s.shape
    heads = columns // HEAD
    blocks = rows // BQ
    e = HEAD**-0.5 * LOG2E
    scores = (sa, sb)
    chips = n // 2
    me = lax.axis_index("tp")
    core, chip = lax.rem(me, 2), lax.div(me, 2)
    after, before, across = (lax.rem(chip + d, chips) for d in (1, chips - 1, 2))
    right, left, partner = 2 * after + core, 2 * before + core, 2 * chip + 1 - core
    part = BQ // n
    early, late = pl.ds(0, part // 2), pl.ds(part // 2, part // 2)

    def fetch(i):
        here = pl.ds(i * BQ, BQ)
        return (
            pltpu.make_async_copy(qt_ref.at[:, here], q_s.at[:, here], sems.at[i, 0]),
            pltpu.make_async_copy(k_ref.at[here, :], k_s.at[here, :], sems.at[i, 1]),
            pltpu.make_async_copy(vt_ref.at[:, here], v_s.at[:, here], sems.at[i, 2]),
        )

    def fetch_x(i):
        return pltpu.make_async_copy(x_ref.at[i, core, chip], x_s.at[i], x_sems.at[i])

    get_wo = pltpu.make_async_copy(wo_ref, wo_s, wo_sem)
    for i in range(blocks):
        for copy in fetch(i):
            copy.start()
        if i == 0:
            get_wo.start()
    for i in range(blocks):
        fetch_x(i).start()

    barrier = pltpu.get_barrier_semaphore()
    for other in (left, right, partner):
        pl.semaphore_signal(barrier, inc=1, device_id={"tp": other}, device_id_type=pl.DeviceIdType.MESH)
    pl.semaphore_wait(barrier, 3)

    def remote(c, kind, src, dst, to):
        return pltpu.make_async_remote_copy(src, dst, send_sems.at[c, kind], recv_sems.at[c, kind], device_id={"tp": to},
                                            device_id_type=pl.DeviceIdType.MESH)

    def copies(c):
        mine, other = y_s.at[c, core], y_s.at[c, core]
        return {
            0: (give_s.at[c], take_s.at[c], partner),
            1: (far_out.at[c, 0], far_in.at[c, 0], right),
            2: (far_out.at[c, 1], far_in.at[c, 1], left),
            3: (near_out.at[c, 0], near_in.at[c, 0], right),
            4: (near_out.at[c, 1], near_in.at[c, 1], left),
            5: (mine.at[chip], other.at[chip], right),
            6: (mine.at[chip], other.at[chip], left),
            7: (mine.at[chip], other.at[chip], partner),
            8: (mine.at[before, early], other.at[before, early], right),
            9: (mine.at[after, late], other.at[after, late], left),
            10: (mine.at[before], other.at[before], partner),
            11: (mine.at[after], other.at[after], partner),
            12: (mine.at[across], other.at[across], partner),
        }

    def start(c, *kinds):
        for kind in kinds:
            remote(c, kind, *copies(c)[kind]).start()

    def arrived(c, *kinds):
        for kind in kinds:
            remote(c, kind, *copies(c)[kind]).wait_recv()

    f32, bf16 = jnp.float32, jnp.bfloat16

    def stage(c, s):
        if s == 0:
            start(c, 0)
        if s == 1:
            arrived(c, 0)
            for q in range(chips):
                sum_s[c, q] = sum_s[c, q] + take_s[c, q].astype(f32)
            far_out[c, 0] = sum_s[c, across, early, :].astype(bf16)
            far_out[c, 1] = sum_s[c, across, late, :].astype(bf16)
            start(c, 1, 2)
        if s == 2:
            arrived(c, 1, 2)
            near_out[c, 0, early, :] = (sum_s[c, after, early, :] + far_in[c, 0].astype(f32)).astype(bf16)
            near_out[c, 0, late, :] = sum_s[c, after, late, :].astype(bf16)
            near_out[c, 1, early, :] = sum_s[c, before, early, :].astype(bf16)
            near_out[c, 1, late, :] = (sum_s[c, before, late, :] + far_in[c, 1].astype(f32)).astype(bf16)
            start(c, 3, 4)
        if s == 3:
            arrived(c, 3, 4)
            fetch_x(c).wait()
            total = sum_s[c, chip] + near_in[c, 0].astype(f32) + near_in[c, 1].astype(f32)
            y_s[c, core, chip] = (x_s[c].astype(f32) + total).astype(bf16)
            start(c, 5, 6, 7)
        if s == 4:
            arrived(c, 5, 6, 7)
            start(c, 8, 9, 10, 11)
        if s == 5:
            arrived(c, 8, 9, 10, 11)
            start(c, 12)
        if s == 6:
            arrived(c, 12)

    last_stage = 6
    flight = []

    clock = [0.0]

    def due(spent=None):
        clock[0] += spent or 0
        now = [(c, s) for c, s, ready in flight if spent is None or ready <= clock[0]]
        flight[:] = [(c, s + 1, clock[0] + TRAVEL[s]) if (c, s) in now else (c, s, ready) for c, s, ready in flight if (c, s) not in now or s < last_stage]
        return now

    def run(now):
        for c, s in now:
            stage(c, s)

    ones = jnp.ones((16, BQ), bf16)
    half = BQ // 2
    my_rows, other_rows = pl.multiple_of(core * half, half), pl.multiple_of((1 - core) * half, half)

    def column(h):
        return pl.ds(pl.multiple_of(h * HEAD, HEAD), HEAD)

    for iq in range(blocks):
        here = pl.ds(iq * BQ, BQ)
        for copy in fetch(iq):
            copy.wait()
        tiles = iq + 1
        unroll = max(4, min(heads, 16 // tiles))
        unroll = max(u for u in (16, 8, 4, 2) if u <= unroll and heads % u == 0)

        def first(h, s_ref, j):
            tile = pl.ds(j * BQ, BQ)
            s = dot(k_s[tile, column(h)], q_s[column(h), here])
            if j == iq:
                seen = lax.broadcasted_iota(jnp.int32, (BQ, BQ), 0) <= lax.broadcasted_iota(jnp.int32, (BQ, BQ), 1)
                s = jnp.where(seen, s, HIDDEN)
            s_ref[tile, :] = s
            return s.reshape(BQ // 8, 8, BQ).max(0)

        def second(h, s_ref, j, top):
            tile = pl.ds(j * BQ, BQ)
            p = jnp.exp2((s_ref[tile, :] - top) * e).astype(bf16)
            return dot(jnp.concatenate([v_s[column(h), tile], ones], 0), p)

        def peak(parts):
            m = parts[0]
            for part in parts[1:]:
                m = jnp.maximum(m, part)
            return m.max(axis=0, keepdims=True)

        def finish(h, total):
            done = (total[:HEAD] * (1 / total[HEAD : HEAD + 1])).astype(bf16).T
            seen_s[pl.ds(my_rows, half), column(h)] = done[:half]
            seen_s[pl.ds(other_rows, half), column(h)] = done[half:]

        plan = [due(unroll * (0.22 + 0.06 * tiles)) for _ in range(heads // unroll)]

        def group(g, top):
            for u in range(unroll):
                h = g * unroll + u
                later = jnp.minimum(h + 1, heads - 1)
                parts, total = [], None
                for j in range(tiles):
                    parts.append(first(later, scores[(u + 1) % 2], j))
                    got = second(h, scores[u % 2], j, top)
                    total = got if total is None else total + got
                finish(h, total)
                top = peak(parts)
            for i, now in enumerate(plan):
                if now:
                    pl.when(g == i)(functools.partial(run, now))
            return top

        top = peak([first(0, scores[0], j) for j in range(tiles)])
        lax.fori_loop(0, heads // unroll, group, top)
        if iq == 0:
            get_wo.wait()
        term = dot(seen_s[...], wo_s[...])
        for q in range(chips):
            sum_s[iq, q] = term[q * part : (q + 1) * part]
            give_s[iq, q] = term[half + q * part : half + (q + 1) * part].astype(bf16)
        clock[0] += 1.2
        flight.append((iq, 0, clock[0]))
        run(due(0))

    while flight:
        run(due())
    for c in range(blocks):
        for kind, copy in copies(c).items():
            remote(c, kind, *copy).wait_send()


def attend(n, qt, k, vt, wo, x):
    rows, columns = k.shape
    wide = wo.shape[1]
    any_ = pl.BlockSpec(memory_space=pl.ANY)
    bf16, f32 = jnp.bfloat16, jnp.float32
    blocks, chips, part = rows // BQ, n // 2, BQ // n
    cut = (blocks, 2, chips, part, wide)
    kinds = 13
    y = pl.pallas_call(
        functools.partial(attend_kernel, n),
        in_specs=[any_] * 5,
        out_specs=pl.BlockSpec(memory_space=pltpu.VMEM),
        out_shape=pltpu.VMEM(cut, bf16),
        scratch_shapes=[
            pltpu.VMEM((columns, rows), bf16),
            pltpu.VMEM((rows, columns), bf16),
            pltpu.VMEM((columns, rows), bf16),
            pltpu.VMEM(wo.shape, bf16),
            pltpu.VMEM((rows, BQ), f32),
            pltpu.VMEM((rows, BQ), f32),
            pltpu.VMEM((BQ, columns), bf16),
            pltpu.VMEM((blocks, chips, part, wide), f32),
            pltpu.VMEM((blocks, part, wide), bf16),
            pltpu.VMEM((blocks, chips, part, wide), bf16),
            pltpu.VMEM((blocks, chips, part, wide), bf16),
            pltpu.VMEM((blocks, 2, part // 2, wide), bf16),
            pltpu.VMEM((blocks, 2, part // 2, wide), bf16),
            pltpu.VMEM((blocks, 2, part, wide), bf16),
            pltpu.VMEM((blocks, 2, part, wide), bf16),
            pltpu.SemaphoreType.DMA((blocks, 3)),
            pltpu.SemaphoreType.DMA,
            pltpu.SemaphoreType.DMA((blocks,)),
            pltpu.SemaphoreType.DMA((blocks, kinds)),
            pltpu.SemaphoreType.DMA((blocks, kinds)),
        ],
        compiler_params=pltpu.CompilerParams(vmem_limit_bytes=VMEM - 8 * 2**20, collective_id=0, has_side_effects=True),
        cost_estimate=pl.CostEstimate(flops=2 * rows * rows * columns + 2 * rows * wide * columns, transcendentals=rows * rows * columns // HEAD // 2, bytes_accessed=8 * rows * columns),
    )(qt, k, vt, wo, x.reshape(cut))
    return y.reshape(rows, wide)


def solution(mesh):
    n = mesh.shape["tp"]

    def step(x, gain, wq, wk, wv, wo):
        qt, k, vt = project(x, gain, wq, wk, wv)
        return attend(n, qt, k, vt, wo, x)

    tokens, columns = P("dp", None), P(None, "tp")
    return jax.shard_map(
        step,
        mesh=mesh,
        in_specs=(tokens, P(None), columns, columns, columns, P("tp", None)),
        out_specs=tokens,
        check_vma=False,
    )
```

```python
import functools

import jax
import jax.numpy as jnp
import numpy as np
from jax import lax
from jax.experimental import pallas as pl
from jax.experimental.pallas import tpu as pltpu
from jax.sharding import PartitionSpec as P

HEAD = 128
THETA = 10000
HIDDEN = -2e30
LOG2E = 1.4426950408889634
VMEM = 60 * 2**20
COLS = 512
ROWS = 256
BQ = 256
TRAVEL = (2.2, 3.8, 4.6, 4.6, 3.8, 2.2, 0)


def dot(a, b):
    return lax.dot_general(a, b, (((1,), (0,)), ((), ())), preferred_element_type=jnp.float32)


def table(rows):
    half = HEAD // 2
    angle = np.arange(rows, dtype=np.float32)[:, None] * (np.float32(THETA) ** (-np.arange(half, dtype=np.float32) / half)).astype(np.float32)
    return np.concatenate([np.cos(angle.astype(np.float64)), np.sin(angle.astype(np.float64))], -1).astype(np.float32)


def project_kernel(x_ref, gain_ref, cs_ref, wq_ref, wk_ref, wv_ref, qt_ref, k_ref, vt_ref, some_s, cos_s, sin_s, flat_s, tall_s, sems):
    n = pl.program_id(0)
    rows = some_s.shape[1]
    per = pl.num_programs(0) // 3
    slot = lax.rem(n, 2)
    step = COLS // HEAD

    @pl.when(n == 0)
    def _():
        gain = gain_ref[...].astype(jnp.float32).reshape(1, -1)
        low = lax.broadcasted_iota(jnp.int32, (HEAD, HEAD), 1) < HEAD // 2

        def prepare(i, _):
            here = pl.ds(i * HEAD, HEAD)
            wide = x_ref[here, :].astype(jnp.float32)
            scale = lax.rsqrt(jnp.mean(wide * wide, -1, keepdims=True) + 1e-6)
            normed = (wide * scale * gain).astype(jnp.bfloat16)
            for d in range(some_s.shape[0]):
                some_s[d, here, :] = normed[:, d * HEAD : (d + 1) * HEAD]
            cs = cs_ref[here, :]
            other = pltpu.roll(cs, HEAD // 2, 1)
            cos_s[here, :] = jnp.where(low, cs, other)
            sin_s[here, :] = jnp.where(low, -other, cs)

        lax.fori_loop(0, rows // HEAD, prepare, None)

    def turned(t, here):
        t = t.astype(jnp.bfloat16).astype(jnp.float32)
        return (t * cos_s[here, :] + pltpu.roll(t, HEAD // 2, 1) * sin_s[here, :]).astype(jnp.bfloat16)

    def flat_out(i, s, ref):
        return pltpu.make_async_copy(flat_s.at[s], ref.at[:, pl.ds(i * step, step)], sems.at[s])

    def tall_out(i, s):
        return pltpu.make_async_copy(tall_s.at[s], k_ref.at[pl.ds(i * step, step)], sems.at[s])

    @pl.when((n >= 2) & (n < per + 2))
    def _():
        flat_out(n - 2, slot, qt_ref).wait()

    @pl.when((n >= per + 2) & (n < 2 * per + 2))
    def _():
        tall_out(n - 2 - per, slot).wait()

    @pl.when(n >= 2 * per + 2)
    def _():
        flat_out(n - 2 - 2 * per, slot, vt_ref).wait()

    def multiply(w_ref, finish):
        before = None
        for at in [*range(0, rows, ROWS), None]:
            t = None
            if at is not None:
                t = dot(jnp.concatenate([some_s[d, at : at + ROWS, :] for d in range(some_s.shape[0])], 1), w_ref[...])
            if before is not None:
                start, done = before
                for r in range(0, ROWS, HEAD):
                    for h in range(step):
                        finish(done[r : r + HEAD, h * HEAD : (h + 1) * HEAD], start + r, h)
            before = at, t

    @pl.when(n < per)
    def _():
        def finish(t, at, h):
            flat_s[slot, at // HEAD, h] = turned(t, pl.ds(at, HEAD)).T

        multiply(wq_ref, finish)
        flat_out(n, slot, qt_ref).start()

    @pl.when((n >= per) & (n < 2 * per))
    def _():
        def finish(t, at, h):
            tall_s[slot, h, at : at + HEAD, :] = turned(t, pl.ds(at, HEAD))

        multiply(wk_ref, finish)
        tall_out(n - per, slot).start()

    @pl.when(n >= 2 * per)
    def _():
        def finish(t, at, h):
            flat_s[slot, at // HEAD, h] = t.astype(jnp.bfloat16).T

        multiply(wv_ref, finish)
        flat_out(n - 2 * per, slot, vt_ref).start()

    @pl.when(n == 3 * per - 1)
    def _():
        flat_out(n - 1 - 2 * per, 1 - slot, vt_ref).wait()
        flat_out(n - 2 * per, slot, vt_ref).wait()


def project(x, gain, wq, wk, wv):
    rows, wide = x.shape
    columns = wq.shape[1]
    heads = columns // HEAD
    per = columns // COLS
    whole = lambda n: (0, 0)
    one = pl.Buffered(buffer_count=1)
    weight = lambda k: pl.BlockSpec((wide, COLS), lambda n: (0, jnp.clip(n - k * per, 0, per - 1)))
    any_ = pl.BlockSpec(memory_space=pl.ANY)
    return pl.pallas_call(
        project_kernel,
        grid=(3 * per,),
        in_specs=[
            pl.BlockSpec((rows, wide), whole, pipeline_mode=one),
            pl.BlockSpec((wide,), lambda n: (0,), pipeline_mode=one),
            pl.BlockSpec((rows, HEAD), whole, pipeline_mode=one),
            weight(0), weight(1), weight(2),
        ],
        out_specs=[any_, any_, any_],
        out_shape=[
            jax.ShapeDtypeStruct((rows // HEAD, heads, HEAD, HEAD), jnp.bfloat16),
            jax.ShapeDtypeStruct((heads, rows, HEAD), jnp.bfloat16),
            jax.ShapeDtypeStruct((rows // HEAD, heads, HEAD, HEAD), jnp.bfloat16),
        ],
        scratch_shapes=[
            pltpu.VMEM((wide // HEAD, rows, HEAD), jnp.bfloat16),
            pltpu.VMEM((rows, HEAD), jnp.float32),
            pltpu.VMEM((rows, HEAD), jnp.float32),
            pltpu.VMEM((2, rows // HEAD, COLS // HEAD, HEAD, HEAD), jnp.bfloat16),
            pltpu.VMEM((2, COLS // HEAD, rows, HEAD), jnp.bfloat16),
            pltpu.SemaphoreType.DMA((2,)),
        ],
        compiler_params=pltpu.CompilerParams(dimension_semantics=("arbitrary",), vmem_limit_bytes=VMEM),
        cost_estimate=pl.CostEstimate(flops=6 * rows * wide * columns, transcendentals=0, bytes_accessed=6 * wide * columns + 6 * rows * columns),
    )(x, gain, jnp.asarray(table(rows)), wq, wk, wv)


def attend_kernel(n, qt_ref, k_ref, vt_ref, wo_ref, x_ref, y_s, q_s, k_s, v_s, wo_s, sa, sb, seen_s, sum_s, x_s,
                  give_s, take_s, far_out, far_in, near_out, near_in, sems, wo_sems, x_sems, send_sems, recv_sems):
    heads, rows, _ = k_s.shape
    blocks = rows // BQ
    per = BQ // HEAD
    e = HEAD**-0.5 * LOG2E
    scores = (sa, sb)
    chips = n // 2
    me = lax.axis_index("tp")
    core, chip = lax.rem(me, 2), lax.div(me, 2)
    after, before, across = (lax.rem(chip + d, chips) for d in (1, chips - 1, 2))
    right, left, partner = 2 * after + core, 2 * before + core, 2 * chip + 1 - core
    part = BQ // n
    early, late = pl.ds(0, part // 2), pl.ds(part // 2, part // 2)

    def fetch(i):
        here, tiles = pl.ds(i * BQ, BQ), pl.ds(i * per, per)
        return (
            pltpu.make_async_copy(qt_ref.at[tiles], q_s.at[tiles], sems.at[i, 0]),
            pltpu.make_async_copy(k_ref.at[:, here], k_s.at[:, here], sems.at[i, 1]),
            pltpu.make_async_copy(vt_ref.at[tiles], v_s.at[tiles], sems.at[i, 2]),
        )

    def fetch_x(i):
        return pltpu.make_async_copy(x_ref.at[i, core, chip], x_s.at[i], x_sems.at[i])

    get_wo = [pltpu.make_async_copy(wo_ref.at[:, pl.ds(c * HEAD, HEAD)], wo_s.at[c], wo_sems.at[c]) for c in range(wo_s.shape[0])]
    for copy in [*fetch(0), *get_wo, *fetch(1)]:
        copy.start()
    for i in range(blocks):
        fetch_x(i).start()

    barrier = pltpu.get_barrier_semaphore()
    for other in (left, right, partner):
        pl.semaphore_signal(barrier, inc=1, device_id={"tp": other}, device_id_type=pl.DeviceIdType.MESH)
    pl.semaphore_wait(barrier, 3)

    def remote(c, kind, src, dst, to):
        return pltpu.make_async_remote_copy(src, dst, send_sems.at[c, kind], recv_sems.at[c, kind], device_id={"tp": to},
                                            device_id_type=pl.DeviceIdType.MESH)

    def copies(c):
        mine, other = y_s.at[c, core], y_s.at[c, core]
        return {
            0: (give_s.at[c], take_s.at[c], partner),
            1: (far_out.at[c, 0], far_in.at[c, 0], right),
            2: (far_out.at[c, 1], far_in.at[c, 1], left),
            3: (near_out.at[c, 0], near_in.at[c, 0], right),
            4: (near_out.at[c, 1], near_in.at[c, 1], left),
            5: (mine.at[chip], other.at[chip], right),
            6: (mine.at[chip], other.at[chip], left),
            7: (mine.at[chip], other.at[chip], partner),
            8: (mine.at[before, early], other.at[before, early], right),
            9: (mine.at[after, late], other.at[after, late], left),
            10: (mine.at[before], other.at[before], partner),
            11: (mine.at[after], other.at[after], partner),
            12: (mine.at[across], other.at[across], partner),
        }

    def start(c, *kinds):
        for kind in kinds:
            remote(c, kind, *copies(c)[kind]).start()

    def arrived(c, *kinds):
        for kind in kinds:
            remote(c, kind, *copies(c)[kind]).wait_recv()

    f32, bf16 = jnp.float32, jnp.bfloat16

    def stage(c, s):
        if s == 0:
            start(c, 0)
        if s == 1:
            arrived(c, 0)
            for q in range(chips):
                sum_s[c, q] = sum_s[c, q] + take_s[c, q].astype(f32)
            far_out[c, 0] = sum_s[c, across, early, :].astype(bf16)
            far_out[c, 1] = sum_s[c, across, late, :].astype(bf16)
            start(c, 1, 2)
        if s == 2:
            arrived(c, 1, 2)
            near_out[c, 0, early, :] = (sum_s[c, after, early, :] + far_in[c, 0].astype(f32)).astype(bf16)
            near_out[c, 0, late, :] = sum_s[c, after, late, :].astype(bf16)
            near_out[c, 1, early, :] = sum_s[c, before, early, :].astype(bf16)
            near_out[c, 1, late, :] = (sum_s[c, before, late, :] + far_in[c, 1].astype(f32)).astype(bf16)
            start(c, 3, 4)
        if s == 3:
            arrived(c, 3, 4)
            fetch_x(c).wait()
            total = sum_s[c, chip] + near_in[c, 0].astype(f32) + near_in[c, 1].astype(f32)
            y_s[c, core, chip] = (x_s[c].astype(f32) + total).astype(bf16)
            start(c, 5, 6, 7)
        if s == 4:
            arrived(c, 5, 6, 7)
            start(c, 8, 9, 10, 11)
        if s == 5:
            arrived(c, 8, 9, 10, 11)
            start(c, 12)
        if s == 6:
            arrived(c, 12)

    last_stage = 6
    flight = []

    clock = [0.0]

    def due(spent=None):
        clock[0] += spent or 0
        now = [(c, s) for c, s, ready in flight if spent is None or ready <= clock[0]]
        flight[:] = [(c, s + 1, clock[0] + TRAVEL[s]) if (c, s) in now else (c, s, ready) for c, s, ready in flight if (c, s) not in now or s < last_stage]
        return now

    def run(now):
        for c, s in now:
            stage(c, s)

    ones = jnp.ones((16, BQ), bf16)
    half = BQ // 2
    my_rows, other_rows = pl.multiple_of(core * half, half), pl.multiple_of((1 - core) * half, half)

    for iq in range(blocks):
        for copy in fetch(iq):
            copy.wait()
        if iq + 2 < blocks:
            for copy in fetch(iq + 2):
                copy.start()
        tiles = iq + 1
        unroll = max(4, min(heads, 16 // tiles))
        unroll = max(u for u in (16, 8, 4, 2) if u <= unroll and heads % u == 0)

        def first(h, s_ref, j):
            tile = pl.ds(j * BQ, BQ)
            s = dot(k_s[h, tile, :], jnp.concatenate([q_s[iq * per + i, h] for i in range(per)], 1))
            if j == iq:
                seen = lax.broadcasted_iota(jnp.int32, (BQ, BQ), 0) <= lax.broadcasted_iota(jnp.int32, (BQ, BQ), 1)
                s = jnp.where(seen, s, HIDDEN)
            s_ref[tile, :] = s
            return s.reshape(BQ // 8, 8, BQ).max(0)

        def second(h, s_ref, j, top):
            tile = pl.ds(j * BQ, BQ)
            p = jnp.exp2((s_ref[tile, :] - top) * e).astype(bf16)
            values = jnp.concatenate([v_s[j * per + i, h] for i in range(per)], 1)
            return dot(jnp.concatenate([values, ones], 0), p)

        def peak(parts):
            m = parts[0]
            for part in parts[1:]:
                m = jnp.maximum(m, part)
            return m.max(axis=0, keepdims=True)

        def finish(h, total):
            done = (total[:HEAD] * (1 / total[HEAD : HEAD + 1])).astype(bf16).T
            seen_s[h, pl.ds(my_rows, half), :] = done[:half]
            seen_s[h, pl.ds(other_rows, half), :] = done[half:]

        plan = [due(unroll * (0.22 + 0.06 * tiles)) for _ in range(heads // unroll)]

        def group(g, top):
            for u in range(unroll):
                h = g * unroll + u
                later = jnp.minimum(h + 1, heads - 1)
                parts, total = [], None
                for j in range(tiles):
                    parts.append(first(later, scores[(u + 1) % 2], j))
                    got = second(h, scores[u % 2], j, top)
                    total = got if total is None else total + got
                finish(h, total)
                top = peak(parts)
            for i, now in enumerate(plan):
                if now:
                    pl.when(g == i)(functools.partial(run, now))
            return top

        top = peak([first(0, scores[0], j) for j in range(tiles)])
        lax.fori_loop(0, heads // unroll, group, top)
        if iq == 0:
            for copy in get_wo:
                copy.wait()
        term = dot(jnp.concatenate([seen_s[h] for h in range(heads)], 1), jnp.concatenate([wo_s[c] for c in range(wo_s.shape[0])], 1))
        for q in range(chips):
            sum_s[iq, q] = term[q * part : (q + 1) * part]
            give_s[iq, q] = term[half + q * part : half + (q + 1) * part].astype(bf16)
        clock[0] += 1.2
        flight.append((iq, 0, clock[0]))
        run(due(0))

    while flight:
        run(due())
    for c in range(blocks):
        for kind, copy in copies(c).items():
            remote(c, kind, *copy).wait_send()


def attend(n, qt, k, vt, wo, x):
    heads, rows, _ = k.shape
    columns, wide = wo.shape
    any_ = pl.BlockSpec(memory_space=pl.ANY)
    bf16, f32 = jnp.bfloat16, jnp.float32
    blocks, chips, part = rows // BQ, n // 2, BQ // n
    cut = (blocks, 2, chips, part, wide)
    kinds = 13
    y = pl.pallas_call(
        functools.partial(attend_kernel, n),
        in_specs=[any_] * 5,
        out_specs=pl.BlockSpec(memory_space=pltpu.VMEM),
        out_shape=pltpu.VMEM(cut, bf16),
        scratch_shapes=[
            pltpu.VMEM(qt.shape, bf16),
            pltpu.VMEM(k.shape, bf16),
            pltpu.VMEM(vt.shape, bf16),
            pltpu.VMEM((wide // HEAD, columns, HEAD), bf16),
            pltpu.VMEM((rows, BQ), f32),
            pltpu.VMEM((rows, BQ), f32),
            pltpu.VMEM((heads, BQ, HEAD), bf16),
            pltpu.VMEM((blocks, chips, part, wide), f32),
            pltpu.VMEM((blocks, part, wide), bf16),
            pltpu.VMEM((blocks, chips, part, wide), bf16),
            pltpu.VMEM((blocks, chips, part, wide), bf16),
            pltpu.VMEM((blocks, 2, part // 2, wide), bf16),
            pltpu.VMEM((blocks, 2, part // 2, wide), bf16),
            pltpu.VMEM((blocks, 2, part, wide), bf16),
            pltpu.VMEM((blocks, 2, part, wide), bf16),
            pltpu.SemaphoreType.DMA((blocks, 3)),
            pltpu.SemaphoreType.DMA((wide // HEAD,)),
            pltpu.SemaphoreType.DMA((blocks,)),
            pltpu.SemaphoreType.DMA((blocks, kinds)),
            pltpu.SemaphoreType.DMA((blocks, kinds)),
        ],
        compiler_params=pltpu.CompilerParams(vmem_limit_bytes=VMEM - 8 * 2**20, collective_id=0, has_side_effects=True),
        cost_estimate=pl.CostEstimate(flops=2 * rows * rows * columns + 2 * rows * wide * columns, transcendentals=rows * rows * columns // HEAD // 2, bytes_accessed=8 * rows * columns),
    )(qt, k, vt, wo, x.reshape(cut))
    return y.reshape(rows, wide)


def solution(mesh):
    n = mesh.shape["tp"]

    def step(x, gain, wq, wk, wv, wo):
        qt, k, vt = project(x, gain, wq, wk, wv)
        return attend(n, qt, k, vt, wo, x)

    tokens, columns = P("dp", None), P(None, "tp")
    return jax.shard_map(
        step,
        mesh=mesh,
        in_specs=(tokens, P(None), columns, columns, columns, P("tp", None)),
        out_specs=tokens,
        check_vma=False,
    )
```

```python
import functools

import jax
import jax.numpy as jnp
import numpy as np
from jax import lax
from jax.experimental import pallas as pl
from jax.experimental.pallas import tpu as pltpu
from jax.sharding import PartitionSpec as P

HEAD = 128
THETA = 10000
HIDDEN = -2e30
LOG2E = 1.4426950408889634
VMEM = 60 * 2**20
COLS = 512
ROWS = 256
BQ = 256
TRAVEL = (2.2, 3.8, 4.6, 4.6, 3.8, 2.2, 0)


def dot(a, b):
    return lax.dot_general(a, b, (((1,), (0,)), ((), ())), preferred_element_type=jnp.float32)


def table(rows):
    half = HEAD // 2
    angle = np.arange(rows, dtype=np.float32)[:, None] * (np.float32(THETA) ** (-np.arange(half, dtype=np.float32) / half)).astype(np.float32)
    return np.concatenate([np.cos(angle.astype(np.float64)), np.sin(angle.astype(np.float64))], -1).astype(np.float32)


def project_kernel(x_ref, gain_ref, cs_ref, wq_ref, wk_ref, wv_ref, qt_ref, k_ref, vt_ref, x_s, cs_s, w_s, some_s, cos_s, sin_s, flat_s, tall_s,
                   sems, x_sems, cs_sems, w_sems):
    n = pl.program_id(0)
    rows = some_s.shape[1]
    per = pl.num_programs(0) // 3
    slot = lax.rem(n, 2)
    step = COLS // HEAD

    def weight(i, ref):
        return pltpu.make_async_copy(ref.at[:, pl.ds(pl.multiple_of(lax.rem(i, per) * COLS, COLS), COLS)], w_s.at[lax.rem(i, 2)], w_sems.at[lax.rem(i, 2)])

    def piece(at):
        here = pl.ds(at, ROWS)
        return (pltpu.make_async_copy(x_ref.at[here, :], x_s.at[here, :], x_sems.at[at // ROWS]),
                pltpu.make_async_copy(cs_ref.at[here, :], cs_s.at[here, :], cs_sems.at[at // ROWS]))

    @pl.when(n == 0)
    def _():
        for at in range(0, rows, ROWS):
            for copy in piece(at):
                copy.start()
            if at == 0:
                weight(0, wq_ref).start()

    for kind, ref in enumerate((wq_ref, wk_ref, wv_ref)):
        pl.when((n + 1 >= kind * per) & (n + 1 < (kind + 1) * per))(lambda ref=ref: weight(n + 1, ref).start())
    weight(n, wq_ref).wait()

    def prepare(at):
        for copy in piece(at):
            copy.wait()
        low = lax.broadcasted_iota(jnp.int32, (HEAD, HEAD), 1) < HEAD // 2
        gain = gain_ref[...].astype(jnp.float32).reshape(1, -1)
        for r in range(at, at + ROWS, HEAD):
            here = pl.ds(r, HEAD)
            wide = x_s[here, :].astype(jnp.float32)
            scale = lax.rsqrt(jnp.mean(wide * wide, -1, keepdims=True) + 1e-6)
            normed = (wide * scale * gain).astype(jnp.bfloat16)
            for d in range(some_s.shape[0]):
                some_s[d, here, :] = normed[:, d * HEAD : (d + 1) * HEAD]
            cs = cs_s[here, :]
            other = pltpu.roll(cs, HEAD // 2, 1)
            cos_s[here, :] = jnp.where(low, cs, other)
            sin_s[here, :] = jnp.where(low, -other, cs)

    def turned(t, here):
        t = t.astype(jnp.bfloat16).astype(jnp.float32)
        return (t * cos_s[here, :] + pltpu.roll(t, HEAD // 2, 1) * sin_s[here, :]).astype(jnp.bfloat16)

    def flat_out(i, s, ref):
        return pltpu.make_async_copy(flat_s.at[s], ref.at[:, pl.ds(i * step, step)], sems.at[s])

    def tall_out(i, s):
        return pltpu.make_async_copy(tall_s.at[s], k_ref.at[pl.ds(i * step, step)], sems.at[s])

    @pl.when((n >= 2) & (n < per + 2))
    def _():
        flat_out(n - 2, slot, qt_ref).wait()

    @pl.when((n >= per + 2) & (n < 2 * per + 2))
    def _():
        tall_out(n - 2 - per, slot).wait()

    @pl.when(n >= 2 * per + 2)
    def _():
        flat_out(n - 2 - 2 * per, slot, vt_ref).wait()

    def multiply(finish, first=False):
        before = None
        if first:
            prepare(0)
        for at in [*range(0, rows, ROWS), None]:
            t = None
            if at is not None:
                if first and at + ROWS < rows:
                    prepare(at + ROWS)
                t = dot(jnp.concatenate([some_s[d, at : at + ROWS, :] for d in range(some_s.shape[0])], 1), w_s[slot])
            if before is not None:
                start, done = before
                for r in range(0, ROWS, HEAD):
                    for h in range(step):
                        finish(done[r : r + HEAD, h * HEAD : (h + 1) * HEAD], start + r, h)
            before = at, t

    def query(t, at, h):
        flat_s[slot, at // HEAD, h] = turned(t, pl.ds(at, HEAD)).T

    @pl.when(n == 0)
    def _():
        multiply(query, first=True)
        flat_out(n, slot, qt_ref).start()

    @pl.when((n > 0) & (n < per))
    def _():
        multiply(query)
        flat_out(n, slot, qt_ref).start()

    @pl.when((n >= per) & (n < 2 * per))
    def _():
        def finish(t, at, h):
            tall_s[slot, h, at : at + HEAD, :] = turned(t, pl.ds(at, HEAD))

        multiply(finish)
        tall_out(n - per, slot).start()

    @pl.when(n >= 2 * per)
    def _():
        def finish(t, at, h):
            flat_s[slot, at // HEAD, h] = t.astype(jnp.bfloat16).T

        multiply(finish)
        flat_out(n - 2 * per, slot, vt_ref).start()

    @pl.when(n == 3 * per - 1)
    def _():
        flat_out(n - 1 - 2 * per, 1 - slot, vt_ref).wait()
        flat_out(n - 2 * per, slot, vt_ref).wait()


def project(x, gain, wq, wk, wv):
    rows, wide = x.shape
    columns = wq.shape[1]
    heads = columns // HEAD
    per = columns // COLS
    any_ = pl.BlockSpec(memory_space=pl.ANY)
    return pl.pallas_call(
        project_kernel,
        grid=(3 * per,),
        in_specs=[any_, pl.BlockSpec((wide,), lambda n: (0,), pipeline_mode=pl.Buffered(buffer_count=1)), any_, any_, any_, any_],
        out_specs=[any_, any_, any_],
        out_shape=[
            jax.ShapeDtypeStruct((rows // HEAD, heads, HEAD, HEAD), jnp.bfloat16),
            jax.ShapeDtypeStruct((heads, rows, HEAD), jnp.bfloat16),
            jax.ShapeDtypeStruct((rows // HEAD, heads, HEAD, HEAD), jnp.bfloat16),
        ],
        scratch_shapes=[
            pltpu.VMEM((rows, wide), jnp.bfloat16),
            pltpu.VMEM((rows, HEAD), jnp.float32),
            pltpu.VMEM((2, wide, COLS), jnp.bfloat16),
            pltpu.VMEM((wide // HEAD, rows, HEAD), jnp.bfloat16),
            pltpu.VMEM((rows, HEAD), jnp.float32),
            pltpu.VMEM((rows, HEAD), jnp.float32),
            pltpu.VMEM((2, rows // HEAD, COLS // HEAD, HEAD, HEAD), jnp.bfloat16),
            pltpu.VMEM((2, COLS // HEAD, rows, HEAD), jnp.bfloat16),
            pltpu.SemaphoreType.DMA((2,)),
            pltpu.SemaphoreType.DMA((rows // ROWS,)),
            pltpu.SemaphoreType.DMA((rows // ROWS,)),
            pltpu.SemaphoreType.DMA((2,)),
        ],
        compiler_params=pltpu.CompilerParams(dimension_semantics=("arbitrary",), vmem_limit_bytes=VMEM),
        cost_estimate=pl.CostEstimate(flops=6 * rows * wide * columns, transcendentals=0, bytes_accessed=6 * wide * columns + 6 * rows * columns),
    )(x, gain, jnp.asarray(table(rows)), wq, wk, wv)


def attend_kernel(n, qt_ref, k_ref, vt_ref, wo_ref, x_ref, y_s, q_s, k_s, v_s, wo_s, sa, sb, seen_a, seen_b, sum_s, x_s,
                  give_s, take_s, far_out, far_in, near_out, near_in, sems, wo_sems, x_sems, send_sems, recv_sems):
    heads, rows, _ = k_s.shape
    blocks = rows // BQ
    per = BQ // HEAD
    e = HEAD**-0.5 * LOG2E
    scores = (sa, sb)
    seens = (seen_a, seen_b)
    chips = n // 2
    me = lax.axis_index("tp")
    core, chip = lax.rem(me, 2), lax.div(me, 2)
    after, before, across = (lax.rem(chip + d, chips) for d in (1, chips - 1, 2))
    right, left, partner = 2 * after + core, 2 * before + core, 2 * chip + 1 - core
    part = BQ // n
    early, late = pl.ds(0, part // 2), pl.ds(part // 2, part // 2)

    def fetch(i):
        here, tiles = pl.ds(i * BQ, BQ), pl.ds(i * per, per)
        return (
            pltpu.make_async_copy(qt_ref.at[tiles], q_s.at[tiles], sems.at[i, 0]),
            pltpu.make_async_copy(k_ref.at[:, here], k_s.at[:, here], sems.at[i, 1]),
            pltpu.make_async_copy(vt_ref.at[tiles], v_s.at[tiles], sems.at[i, 2]),
        )

    def fetch_x(i):
        return pltpu.make_async_copy(x_ref.at[i, core, chip], x_s.at[i], x_sems.at[i])

    get_wo = [pltpu.make_async_copy(wo_ref.at[:, pl.ds(c * HEAD, HEAD)], wo_s.at[c], wo_sems.at[c]) for c in range(wo_s.shape[0])]
    for copy in [*fetch(0), *get_wo, *fetch(1)]:
        copy.start()
    for i in range(blocks):
        fetch_x(i).start()

    barrier = pltpu.get_barrier_semaphore()
    for other in (left, right, partner):
        pl.semaphore_signal(barrier, inc=1, device_id={"tp": other}, device_id_type=pl.DeviceIdType.MESH)
    pl.semaphore_wait(barrier, 3)

    def remote(c, kind, src, dst, to):
        return pltpu.make_async_remote_copy(src, dst, send_sems.at[c, kind], recv_sems.at[c, kind], device_id={"tp": to},
                                            device_id_type=pl.DeviceIdType.MESH)

    def copies(c):
        mine, other = y_s.at[c, core], y_s.at[c, core]
        return {
            0: (give_s.at[c], take_s.at[c], partner),
            1: (far_out.at[c, 0], far_in.at[c, 0], right),
            2: (far_out.at[c, 1], far_in.at[c, 1], left),
            3: (near_out.at[c, 0], near_in.at[c, 0], right),
            4: (near_out.at[c, 1], near_in.at[c, 1], left),
            5: (mine.at[chip], other.at[chip], right),
            6: (mine.at[chip], other.at[chip], left),
            7: (mine.at[chip], other.at[chip], partner),
            8: (mine.at[before, early], other.at[before, early], right),
            9: (mine.at[after, late], other.at[after, late], left),
            10: (mine.at[before], other.at[before], partner),
            11: (mine.at[after], other.at[after], partner),
            12: (mine.at[across], other.at[across], partner),
        }

    def start(c, *kinds):
        for kind in kinds:
            remote(c, kind, *copies(c)[kind]).start()

    def arrived(c, *kinds):
        for kind in kinds:
            remote(c, kind, *copies(c)[kind]).wait_recv()

    f32, bf16 = jnp.float32, jnp.bfloat16

    def stage(c, s):
        if s == 0:
            start(c, 0)
        if s == 1:
            arrived(c, 0)
            for q in range(chips):
                sum_s[c, q] = sum_s[c, q] + take_s[c, q].astype(f32)
            far_out[c, 0] = sum_s[c, across, early, :].astype(bf16)
            far_out[c, 1] = sum_s[c, across, late, :].astype(bf16)
            start(c, 1, 2)
        if s == 2:
            arrived(c, 1, 2)
            near_out[c, 0, early, :] = (sum_s[c, after, early, :] + far_in[c, 0].astype(f32)).astype(bf16)
            near_out[c, 0, late, :] = sum_s[c, after, late, :].astype(bf16)
            near_out[c, 1, early, :] = sum_s[c, before, early, :].astype(bf16)
            near_out[c, 1, late, :] = (sum_s[c, before, late, :] + far_in[c, 1].astype(f32)).astype(bf16)
            start(c, 3, 4)
        if s == 3:
            arrived(c, 3, 4)
            fetch_x(c).wait()
            total = sum_s[c, chip] + near_in[c, 0].astype(f32) + near_in[c, 1].astype(f32)
            y_s[c, core, chip] = (x_s[c].astype(f32) + total).astype(bf16)
            start(c, 5, 6, 7)
        if s == 4:
            arrived(c, 5, 6, 7)
            start(c, 8, 9, 10, 11)
        if s == 5:
            arrived(c, 8, 9, 10, 11)
            start(c, 12)
        if s == 6:
            arrived(c, 12)

    last_stage = 6
    flight = []

    clock = [0.0]

    def due(spent=None):
        clock[0] += spent or 0
        now = [(c, s) for c, s, ready in flight if spent is None or ready <= clock[0]]
        flight[:] = [(c, s + 1, clock[0] + TRAVEL[s]) if (c, s) in now else (c, s, ready) for c, s, ready in flight if (c, s) not in now or s < last_stage]
        return now

    def run(now):
        for c, s in now:
            stage(c, s)

    ones = jnp.ones((16, BQ), bf16)
    half = BQ // 2
    my_rows, other_rows = pl.multiple_of(core * half, half), pl.multiple_of((1 - core) * half, half)

    def output(c, at, tiles):
        weights = jnp.concatenate([wo_s[at + i] for i in range(tiles)], 1)
        term = dot(jnp.concatenate([seens[c % 2][h] for h in range(heads)], 1), weights)
        columns = pl.ds(pl.multiple_of(at * HEAD, HEAD), tiles * HEAD)
        for q in range(chips):
            sum_s[c, q, :, columns] = term[q * part : (q + 1) * part]
            give_s[c, q, :, columns] = term[half + q * part : half + (q + 1) * part].astype(bf16)

    out_tiles = wo_s.shape[0]
    for iq in range(blocks):
        for copy in fetch(iq):
            copy.wait()
        if iq + 2 < blocks:
            for copy in fetch(iq + 2):
                copy.start()
        tiles = iq + 1
        unroll = max(4, min(heads, 16 // tiles))
        unroll = max(u for u in (16, 8, 4, 2) if u <= unroll and heads % u == 0)

        def first(h, s_ref, j):
            tile = pl.ds(j * BQ, BQ)
            s = dot(k_s[h, tile, :], jnp.concatenate([q_s[iq * per + i, h] for i in range(per)], 1))
            if j == iq:
                seen = lax.broadcasted_iota(jnp.int32, (BQ, BQ), 0) <= lax.broadcasted_iota(jnp.int32, (BQ, BQ), 1)
                s = jnp.where(seen, s, HIDDEN)
            s_ref[tile, :] = s
            return s.reshape(BQ // 8, 8, BQ).max(0)

        def second(h, s_ref, j, top):
            tile = pl.ds(j * BQ, BQ)
            p = jnp.exp2((s_ref[tile, :] - top) * e).astype(bf16)
            values = jnp.concatenate([v_s[j * per + i, h] for i in range(per)], 1)
            return dot(jnp.concatenate([values, ones], 0), p)

        def peak(parts):
            m = parts[0]
            for part in parts[1:]:
                m = jnp.maximum(m, part)
            return m.max(axis=0, keepdims=True)

        def finish(h, total):
            seen_s = seens[iq % 2]
            done = (total[:HEAD] * (1 / total[HEAD : HEAD + 1])).astype(bf16).T
            seen_s[h, pl.ds(my_rows, half), :] = done[:half]
            seen_s[h, pl.ds(other_rows, half), :] = done[half:]

        plan = [due(unroll * (0.22 + 0.06 * tiles) + (0.9 * unroll / heads if 0 < iq < blocks - 1 else 0)) for _ in range(heads // unroll)]

        late_output = 0 < iq < blocks - 1
        groups = heads // unroll

        def group(g, top):
            for u in range(unroll):
                if late_output and u == unroll // 2:
                    output(iq - 1, g * (out_tiles // groups), out_tiles // groups)
                h = g * unroll + u
                later = jnp.minimum(h + 1, heads - 1)
                parts, total = [], None
                for j in range(tiles):
                    parts.append(first(later, scores[(u + 1) % 2], j))
                    got = second(h, scores[u % 2], j, top)
                    total = got if total is None else total + got
                finish(h, total)
                top = peak(parts)
            for i, now in enumerate(plan):
                if now:
                    pl.when(g == i)(functools.partial(run, now))
            return top

        top = peak([first(0, scores[0], j) for j in range(tiles)])
        lax.fori_loop(0, heads // unroll, group, top)
        if iq == 0:
            for copy in get_wo:
                copy.wait()
        if late_output:
            flight.append((iq - 1, 0, clock[0]))
        if iq >= blocks - 2:
            output(iq, 0, out_tiles)
            clock[0] += 1.2
            flight.append((iq, 0, clock[0]))
        run(due(0))

    while flight:
        run(due())
    for c in range(blocks):
        for kind, copy in copies(c).items():
            remote(c, kind, *copy).wait_send()


def attend(n, qt, k, vt, wo, x):
    heads, rows, _ = k.shape
    columns, wide = wo.shape
    any_ = pl.BlockSpec(memory_space=pl.ANY)
    bf16, f32 = jnp.bfloat16, jnp.float32
    blocks, chips, part = rows // BQ, n // 2, BQ // n
    cut = (blocks, 2, chips, part, wide)
    kinds = 13
    y = pl.pallas_call(
        functools.partial(attend_kernel, n),
        in_specs=[any_] * 5,
        out_specs=pl.BlockSpec(memory_space=pltpu.VMEM),
        out_shape=pltpu.VMEM(cut, bf16),
        scratch_shapes=[
            pltpu.VMEM(qt.shape, bf16),
            pltpu.VMEM(k.shape, bf16),
            pltpu.VMEM(vt.shape, bf16),
            pltpu.VMEM((wide // HEAD, columns, HEAD), bf16),
            pltpu.VMEM((rows, BQ), f32),
            pltpu.VMEM((rows, BQ), f32),
            pltpu.VMEM((heads, BQ, HEAD), bf16),
            pltpu.VMEM((heads, BQ, HEAD), bf16),
            pltpu.VMEM((blocks, chips, part, wide), f32),
            pltpu.VMEM((blocks, part, wide), bf16),
            pltpu.VMEM((blocks, chips, part, wide), bf16),
            pltpu.VMEM((blocks, chips, part, wide), bf16),
            pltpu.VMEM((blocks, 2, part // 2, wide), bf16),
            pltpu.VMEM((blocks, 2, part // 2, wide), bf16),
            pltpu.VMEM((blocks, 2, part, wide), bf16),
            pltpu.VMEM((blocks, 2, part, wide), bf16),
            pltpu.SemaphoreType.DMA((blocks, 3)),
            pltpu.SemaphoreType.DMA((wide // HEAD,)),
            pltpu.SemaphoreType.DMA((blocks,)),
            pltpu.SemaphoreType.DMA((blocks, kinds)),
            pltpu.SemaphoreType.DMA((blocks, kinds)),
        ],
        compiler_params=pltpu.CompilerParams(vmem_limit_bytes=VMEM - 8 * 2**20, collective_id=0, has_side_effects=True),
        cost_estimate=pl.CostEstimate(flops=2 * rows * rows * columns + 2 * rows * wide * columns, transcendentals=rows * rows * columns // HEAD // 2, bytes_accessed=8 * rows * columns),
    )(qt, k, vt, wo, x.reshape(cut))
    return y.reshape(rows, wide)


def solution(mesh):
    n = mesh.shape["tp"]

    def step(x, gain, wq, wk, wv, wo):
        qt, k, vt = project(x, gain, wq, wk, wv)
        return attend(n, qt, k, vt, wo, x)

    tokens, columns = P("dp", None), P(None, "tp")
    return jax.shard_map(
        step,
        mesh=mesh,
        in_specs=(tokens, P(None), columns, columns, columns, P("tp", None)),
        out_specs=tokens,
        check_vma=False,
    )
```

```python
import functools

import jax
import jax.numpy as jnp
import numpy as np
from jax import lax
from jax.experimental import pallas as pl
from jax.experimental.pallas import tpu as pltpu
from jax.sharding import PartitionSpec as P

HEAD = 128
THETA = 10000
HIDDEN = -2e30
LOG2E = 1.4426950408889634
VMEM = 60 * 2**20
COLS = 512
ROWS = 256
BQ = 256
TRAVEL = (3, 6, 7, 7, 6, 3, 0)


def dot(a, b):
    return lax.dot_general(a, b, (((1,), (0,)), ((), ())), preferred_element_type=jnp.float32)


def table(rows):
    half = HEAD // 2
    angle = np.arange(rows, dtype=np.float32)[:, None] * (np.float32(THETA) ** (-np.arange(half, dtype=np.float32) / half)).astype(np.float32)
    return np.concatenate([np.cos(angle.astype(np.float64)), np.sin(angle.astype(np.float64))], -1).astype(np.float32)


def project_kernel(x_ref, gain_ref, cs_ref, wq_ref, wk_ref, wv_ref, qt_ref, k_ref, vt_ref, x_s, cs_s, w_s, some_s, cos_s, sin_s, flat_s, tall_s,
                   sems, x_sems, cs_sems, w_sems):
    n = pl.program_id(0)
    rows = some_s.shape[1]
    per = pl.num_programs(0) // 3
    slot = lax.rem(n, 2)
    step = COLS // HEAD

    def weight(i, ref):
        return pltpu.make_async_copy(ref.at[:, pl.ds(pl.multiple_of(lax.rem(i, per) * COLS, COLS), COLS)], w_s.at[lax.rem(i, 2)], w_sems.at[lax.rem(i, 2)])

    def piece(at):
        here = pl.ds(at, ROWS)
        return (pltpu.make_async_copy(x_ref.at[here, :], x_s.at[here, :], x_sems.at[at // ROWS]),
                pltpu.make_async_copy(cs_ref.at[here, :], cs_s.at[here, :], cs_sems.at[at // ROWS]))

    @pl.when(n == 0)
    def _():
        for at in range(0, rows, ROWS):
            for copy in piece(at):
                copy.start()
            if at == 0:
                weight(0, wq_ref).start()

    for kind, ref in enumerate((wq_ref, wk_ref, wv_ref)):
        pl.when((n + 1 >= kind * per) & (n + 1 < (kind + 1) * per))(lambda ref=ref: weight(n + 1, ref).start())
    weight(n, wq_ref).wait()

    def prepare(at):
        for copy in piece(at):
            copy.wait()
        low = lax.broadcasted_iota(jnp.int32, (HEAD, HEAD), 1) < HEAD // 2
        gain = gain_ref[...].astype(jnp.float32).reshape(1, -1)
        for r in range(at, at + ROWS, HEAD):
            here = pl.ds(r, HEAD)
            wide = x_s[here, :].astype(jnp.float32)
            scale = lax.rsqrt(jnp.mean(wide * wide, -1, keepdims=True) + 1e-6)
            normed = (wide * scale * gain).astype(jnp.bfloat16)
            for d in range(some_s.shape[0]):
                some_s[d, here, :] = normed[:, d * HEAD : (d + 1) * HEAD]
            cs = cs_s[here, :]
            other = pltpu.roll(cs, HEAD // 2, 1)
            cos_s[here, :] = jnp.where(low, cs, other)
            sin_s[here, :] = jnp.where(low, -other, cs)

    def turned(t, here):
        t = t.astype(jnp.bfloat16).astype(jnp.float32)
        return (t * cos_s[here, :] + pltpu.roll(t, HEAD // 2, 1) * sin_s[here, :]).astype(jnp.bfloat16)

    def flat_out(i, s, ref):
        return pltpu.make_async_copy(flat_s.at[s], ref.at[:, pl.ds(i * step, step)], sems.at[s])

    def tall_out(i, s):
        return pltpu.make_async_copy(tall_s.at[s], k_ref.at[pl.ds(i * step, step)], sems.at[s])

    @pl.when((n >= 2) & (n < per + 2))
    def _():
        flat_out(n - 2, slot, qt_ref).wait()

    @pl.when((n >= per + 2) & (n < 2 * per + 2))
    def _():
        tall_out(n - 2 - per, slot).wait()

    @pl.when(n >= 2 * per + 2)
    def _():
        flat_out(n - 2 - 2 * per, slot, vt_ref).wait()

    def multiply(finish, first=False):
        before = None
        if first:
            prepare(0)
        for at in [*range(0, rows, ROWS), None]:
            t = None
            if at is not None:
                if first and at + ROWS < rows:
                    prepare(at + ROWS)
                t = dot(jnp.concatenate([some_s[d, at : at + ROWS, :] for d in range(some_s.shape[0])], 1), w_s[slot])
            if before is not None:
                start, done = before
                for r in range(0, ROWS, HEAD):
                    for h in range(step):
                        finish(done[r : r + HEAD, h * HEAD : (h + 1) * HEAD], start + r, h)
            before = at, t

    def query(t, at, h):
        flat_s[slot, at // HEAD, h] = turned(t, pl.ds(at, HEAD)).T

    @pl.when(n == 0)
    def _():
        multiply(query, first=True)
        flat_out(n, slot, qt_ref).start()

    @pl.when((n > 0) & (n < per))
    def _():
        multiply(query)
        flat_out(n, slot, qt_ref).start()

    @pl.when((n >= per) & (n < 2 * per))
    def _():
        def finish(t, at, h):
            tall_s[slot, h, at : at + HEAD, :] = turned(t, pl.ds(at, HEAD))

        multiply(finish)
        tall_out(n - per, slot).start()

    @pl.when(n >= 2 * per)
    def _():
        def finish(t, at, h):
            flat_s[slot, at // HEAD, h] = t.astype(jnp.bfloat16).T

        multiply(finish)
        flat_out(n - 2 * per, slot, vt_ref).start()

    @pl.when(n == 3 * per - 1)
    def _():
        flat_out(n - 1 - 2 * per, 1 - slot, vt_ref).wait()
        flat_out(n - 2 * per, slot, vt_ref).wait()


def project(x, gain, wq, wk, wv):
    rows, wide = x.shape
    columns = wq.shape[1]
    heads = columns // HEAD
    per = columns // COLS
    any_ = pl.BlockSpec(memory_space=pl.ANY)
    return pl.pallas_call(
        project_kernel,
        grid=(3 * per,),
        in_specs=[any_, pl.BlockSpec((wide,), lambda n: (0,), pipeline_mode=pl.Buffered(buffer_count=1)), any_, any_, any_, any_],
        out_specs=[any_, any_, any_],
        out_shape=[
            jax.ShapeDtypeStruct((rows // HEAD, heads, HEAD, HEAD), jnp.bfloat16),
            jax.ShapeDtypeStruct((heads, rows, HEAD), jnp.bfloat16),
            jax.ShapeDtypeStruct((rows // HEAD, heads, HEAD, HEAD), jnp.bfloat16),
        ],
        scratch_shapes=[
            pltpu.VMEM((rows, wide), jnp.bfloat16),
            pltpu.VMEM((rows, HEAD), jnp.float32),
            pltpu.VMEM((2, wide, COLS), jnp.bfloat16),
            pltpu.VMEM((wide // HEAD, rows, HEAD), jnp.bfloat16),
            pltpu.VMEM((rows, HEAD), jnp.float32),
            pltpu.VMEM((rows, HEAD), jnp.float32),
            pltpu.VMEM((2, rows // HEAD, COLS // HEAD, HEAD, HEAD), jnp.bfloat16),
            pltpu.VMEM((2, COLS // HEAD, rows, HEAD), jnp.bfloat16),
            pltpu.SemaphoreType.DMA((2,)),
            pltpu.SemaphoreType.DMA((rows // ROWS,)),
            pltpu.SemaphoreType.DMA((rows // ROWS,)),
            pltpu.SemaphoreType.DMA((2,)),
        ],
        compiler_params=pltpu.CompilerParams(dimension_semantics=("arbitrary",), vmem_limit_bytes=VMEM),
        cost_estimate=pl.CostEstimate(flops=6 * rows * wide * columns, transcendentals=0, bytes_accessed=6 * wide * columns + 6 * rows * columns),
    )(x, gain, jnp.asarray(table(rows)), wq, wk, wv)


def attend_kernel(n, qt_ref, k_ref, vt_ref, wo_ref, x_ref, y_s, q_s, k_s, v_s, wo_s, sa, sb, seen_a, seen_b, sum_s, x_s,
                  give_s, take_s, far_out, far_in, near_out, near_in, sems, wo_sems, x_sems, send_sems, recv_sems):
    heads, rows, _ = k_s.shape
    blocks = rows // BQ
    per = BQ // HEAD
    e = HEAD**-0.5 * LOG2E
    scores = (sa, sb)
    seens = (seen_a, seen_b)
    chips = n // 2
    me = lax.axis_index("tp")
    core, chip = lax.rem(me, 2), lax.div(me, 2)
    after, before, across = (lax.rem(chip + d, chips) for d in (1, chips - 1, 2))
    right, left, partner = 2 * after + core, 2 * before + core, 2 * chip + 1 - core
    part = BQ // n
    early, late = pl.ds(0, part // 2), pl.ds(part // 2, part // 2)

    def fetch(i):
        here, tiles = pl.ds(i * BQ, BQ), pl.ds(i * per, per)
        return (
            pltpu.make_async_copy(qt_ref.at[tiles], q_s.at[tiles], sems.at[i, 0]),
            pltpu.make_async_copy(k_ref.at[:, here], k_s.at[:, here], sems.at[i, 1]),
            pltpu.make_async_copy(vt_ref.at[tiles], v_s.at[tiles], sems.at[i, 2]),
        )

    def fetch_x(i):
        return pltpu.make_async_copy(x_ref.at[i, core, chip], x_s.at[i], x_sems.at[i])

    get_wo = [pltpu.make_async_copy(wo_ref.at[:, pl.ds(c * HEAD, HEAD)], wo_s.at[c], wo_sems.at[c]) for c in range(wo_s.shape[0])]
    for copy in [*fetch(0), *get_wo, *fetch(1)]:
        copy.start()
    for i in range(blocks):
        fetch_x(i).start()

    barrier = pltpu.get_barrier_semaphore()
    for other in (left, right, partner):
        pl.semaphore_signal(barrier, inc=1, device_id={"tp": other}, device_id_type=pl.DeviceIdType.MESH)
    pl.semaphore_wait(barrier, 3)

    def remote(c, kind, src, dst, to):
        return pltpu.make_async_remote_copy(src, dst, send_sems.at[c, kind], recv_sems.at[c, kind], device_id={"tp": to},
                                            device_id_type=pl.DeviceIdType.MESH)

    def copies(c):
        mine, other = y_s.at[c, core], y_s.at[c, core]
        return {
            0: (give_s.at[c], take_s.at[c], partner),
            1: (far_out.at[c, 0], far_in.at[c, 0], right),
            2: (far_out.at[c, 1], far_in.at[c, 1], left),
            3: (near_out.at[c, 0], near_in.at[c, 0], right),
            4: (near_out.at[c, 1], near_in.at[c, 1], left),
            5: (mine.at[chip], other.at[chip], right),
            6: (mine.at[chip], other.at[chip], left),
            7: (mine.at[chip], other.at[chip], partner),
            8: (mine.at[before, early], other.at[before, early], right),
            9: (mine.at[after, late], other.at[after, late], left),
            10: (mine.at[before], other.at[before], partner),
            11: (mine.at[after], other.at[after], partner),
            12: (mine.at[across], other.at[across], partner),
        }

    def start(c, *kinds):
        for kind in kinds:
            remote(c, kind, *copies(c)[kind]).start()

    def arrived(c, *kinds):
        for kind in kinds:
            remote(c, kind, *copies(c)[kind]).wait_recv()

    f32, bf16 = jnp.float32, jnp.bfloat16

    def stage(c, s):
        if s == 0:
            start(c, 0)
        if s == 1:
            arrived(c, 0)
            for q in range(chips):
                sum_s[c, q] = sum_s[c, q] + take_s[c, q].astype(f32)
            far_out[c, 0] = sum_s[c, across, early, :].astype(bf16)
            far_out[c, 1] = sum_s[c, across, late, :].astype(bf16)
            start(c, 1, 2)
        if s == 2:
            arrived(c, 1, 2)
            near_out[c, 0, early, :] = (sum_s[c, after, early, :] + far_in[c, 0].astype(f32)).astype(bf16)
            near_out[c, 0, late, :] = sum_s[c, after, late, :].astype(bf16)
            near_out[c, 1, early, :] = sum_s[c, before, early, :].astype(bf16)
            near_out[c, 1, late, :] = (sum_s[c, before, late, :] + far_in[c, 1].astype(f32)).astype(bf16)
            start(c, 3, 4)
        if s == 3:
            arrived(c, 3, 4)
            fetch_x(c).wait()
            total = sum_s[c, chip] + near_in[c, 0].astype(f32) + near_in[c, 1].astype(f32)
            y_s[c, core, chip] = (x_s[c].astype(f32) + total).astype(bf16)
            start(c, 5, 6, 7)
        if s == 4:
            arrived(c, 5, 6, 7)
            start(c, 8, 9, 10, 11)
        if s == 5:
            arrived(c, 8, 9, 10, 11)
            start(c, 12)
        if s == 6:
            arrived(c, 12)

    last_stage = 6
    flight = []

    clock = [0.0]

    def due(spent=None):
        clock[0] += spent or 0
        now = [(c, s) for c, s, ready in flight if spent is None or ready <= clock[0]]
        flight[:] = [(c, s + 1, clock[0] + TRAVEL[s]) if (c, s) in now else (c, s, ready) for c, s, ready in flight if (c, s) not in now or s < last_stage]
        return now

    def run(now):
        for c, s in now:
            stage(c, s)

    ones = jnp.ones((16, BQ), bf16)
    half = BQ // 2
    my_rows, other_rows = pl.multiple_of(core * half, half), pl.multiple_of((1 - core) * half, half)

    def output(c, at, tiles):
        weights = jnp.concatenate([wo_s[at + i] for i in range(tiles)], 1)
        term = dot(jnp.concatenate([seens[c % 2][h] for h in range(heads)], 1), weights)
        columns = pl.ds(pl.multiple_of(at * HEAD, HEAD), tiles * HEAD)
        for q in range(chips):
            sum_s[c, q, :, columns] = term[q * part : (q + 1) * part]
            give_s[c, q, :, columns] = term[half + q * part : half + (q + 1) * part].astype(bf16)

    out_tiles = wo_s.shape[0]
    for iq in range(blocks):
        for copy in fetch(iq):
            copy.wait()
        if iq + 2 < blocks:
            for copy in fetch(iq + 2):
                copy.start()
        tiles = iq + 1
        unroll = max(4, min(heads, 16 // tiles))
        unroll = max(u for u in (16, 8, 4, 2) if u <= unroll and heads % u == 0)

        def first(h, s_ref, j):
            tile = pl.ds(j * BQ, BQ)
            s = dot(k_s[h, tile, :], jnp.concatenate([q_s[iq * per + i, h] for i in range(per)], 1))
            if j == iq:
                seen = lax.broadcasted_iota(jnp.int32, (BQ, BQ), 0) <= lax.broadcasted_iota(jnp.int32, (BQ, BQ), 1)
                s = jnp.where(seen, s, HIDDEN)
            s_ref[tile, :] = s
            return s.reshape(BQ // 8, 8, BQ).max(0)

        def second(h, s_ref, j, top):
            tile = pl.ds(j * BQ, BQ)
            p = jnp.exp2((s_ref[tile, :] - top) * e).astype(bf16)
            values = jnp.concatenate([v_s[j * per + i, h] for i in range(per)], 1)
            return dot(jnp.concatenate([values, ones], 0), p)

        def peak(parts):
            m = parts[0]
            for part in parts[1:]:
                m = jnp.maximum(m, part)
            return m.max(axis=0, keepdims=True)

        def finish(h, total):
            seen_s = seens[iq % 2]
            done = (total[:HEAD] * (1 / total[HEAD : HEAD + 1])).astype(bf16).T
            seen_s[h, pl.ds(my_rows, half), :] = done[:half]
            seen_s[h, pl.ds(other_rows, half), :] = done[half:]

        plan = [due(unroll * (0.2 + 0.05 * tiles) + (0.9 * unroll / heads if 0 < iq < blocks - 2 else 0)) for _ in range(heads // unroll)]

        late_output = 0 < iq < blocks - 2
        groups = heads // unroll

        def group(g, top):
            for u in range(unroll):
                if late_output and u == unroll // 2:
                    output(iq - 1, g * (out_tiles // groups), out_tiles // groups)
                h = g * unroll + u
                later = jnp.minimum(h + 1, heads - 1)
                parts, total = [], None
                for j in range(tiles):
                    parts.append(first(later, scores[(u + 1) % 2], j))
                    got = second(h, scores[u % 2], j, top)
                    total = got if total is None else total + got
                finish(h, total)
                top = peak(parts)
            for i, now in enumerate(plan):
                if now:
                    pl.when(g == i)(functools.partial(run, now))
            return top

        top = peak([first(0, scores[0], j) for j in range(tiles)])
        lax.fori_loop(0, heads // unroll, group, top)
        if iq == 0:
            for copy in get_wo:
                copy.wait()
        if late_output:
            flight.append((iq - 1, 0, clock[0]))
        if iq >= blocks - 3:
            output(iq, 0, out_tiles)
            clock[0] += 1.2
            flight.append((iq, 0, clock[0]))
        run(due(0))

    while flight:
        run(due())
    for c in range(blocks):
        for kind, copy in copies(c).items():
            remote(c, kind, *copy).wait_send()


def attend(n, qt, k, vt, wo, x):
    heads, rows, _ = k.shape
    columns, wide = wo.shape
    any_ = pl.BlockSpec(memory_space=pl.ANY)
    bf16, f32 = jnp.bfloat16, jnp.float32
    blocks, chips, part = rows // BQ, n // 2, BQ // n
    cut = (blocks, 2, chips, part, wide)
    kinds = 13
    y = pl.pallas_call(
        functools.partial(attend_kernel, n),
        in_specs=[any_] * 5,
        out_specs=pl.BlockSpec(memory_space=pltpu.VMEM),
        out_shape=pltpu.VMEM(cut, bf16),
        scratch_shapes=[
            pltpu.VMEM(qt.shape, bf16),
            pltpu.VMEM(k.shape, bf16),
            pltpu.VMEM(vt.shape, bf16),
            pltpu.VMEM((wide // HEAD, columns, HEAD), bf16),
            pltpu.VMEM((rows, BQ), f32),
            pltpu.VMEM((rows, BQ), f32),
            pltpu.VMEM((heads, BQ, HEAD), bf16),
            pltpu.VMEM((heads, BQ, HEAD), bf16),
            pltpu.VMEM((blocks, chips, part, wide), f32),
            pltpu.VMEM((blocks, part, wide), bf16),
            pltpu.VMEM((blocks, chips, part, wide), bf16),
            pltpu.VMEM((blocks, chips, part, wide), bf16),
            pltpu.VMEM((blocks, 2, part // 2, wide), bf16),
            pltpu.VMEM((blocks, 2, part // 2, wide), bf16),
            pltpu.VMEM((blocks, 2, part, wide), bf16),
            pltpu.VMEM((blocks, 2, part, wide), bf16),
            pltpu.SemaphoreType.DMA((blocks, 3)),
            pltpu.SemaphoreType.DMA((wide // HEAD,)),
            pltpu.SemaphoreType.DMA((blocks,)),
            pltpu.SemaphoreType.DMA((blocks, kinds)),
            pltpu.SemaphoreType.DMA((blocks, kinds)),
        ],
        compiler_params=pltpu.CompilerParams(vmem_limit_bytes=VMEM - 8 * 2**20, collective_id=0, has_side_effects=True),
        cost_estimate=pl.CostEstimate(flops=2 * rows * rows * columns + 2 * rows * wide * columns, transcendentals=rows * rows * columns // HEAD // 2, bytes_accessed=8 * rows * columns),
    )(qt, k, vt, wo, x.reshape(cut))
    return y.reshape(rows, wide)


def solution(mesh):
    n = mesh.shape["tp"]

    def step(x, gain, wq, wk, wv, wo):
        qt, k, vt = project(x, gain, wq, wk, wv)
        return attend(n, qt, k, vt, wo, x)

    tokens, columns = P("dp", None), P(None, "tp")
    return jax.shard_map(
        step,
        mesh=mesh,
        in_specs=(tokens, P(None), columns, columns, columns, P("tp", None)),
        out_specs=tokens,
        check_vma=False,
    )
```

```python
import functools

import jax
import jax.numpy as jnp
import numpy as np
from jax import lax
from jax.experimental import pallas as pl
from jax.experimental.pallas import tpu as pltpu
from jax.sharding import PartitionSpec as P

HEAD = 128
THETA = 10000
HIDDEN = -2e30
LOG2E = 1.4426950408889634
VMEM = 60 * 2**20
COLS = 512
ROWS = 256
BQ = 256
TRAVEL = (2.2, 3.8, 4.6, 4.6, 3.8, 2.2, 0)


def dot(a, b):
    return lax.dot_general(a, b, (((1,), (0,)), ((), ())), preferred_element_type=jnp.float32)


def table(rows):
    half = HEAD // 2
    angle = np.arange(rows, dtype=np.float32)[:, None] * (np.float32(THETA) ** (-np.arange(half, dtype=np.float32) / half)).astype(np.float32)
    return np.concatenate([np.cos(angle.astype(np.float64)), np.sin(angle.astype(np.float64))], -1).astype(np.float32)


def project_step(n, x_ref, gain_ref, cs_ref, wq_ref, wk_ref, wv_ref, q_s, k_s, v_s, x_s, cs_s, w_s, some_s, cos_s, sin_s, x_sems, cs_sems, w_sems):
    rows = some_s.shape[1]
    per = wq_ref.shape[1] // COLS
    slot = lax.rem(n, 2)
    step = COLS // HEAD

    def weight(i, ref):
        return pltpu.make_async_copy(ref.at[:, pl.ds(pl.multiple_of(lax.rem(i, per) * COLS, COLS), COLS)], w_s.at[lax.rem(i, 2)], w_sems.at[lax.rem(i, 2)])

    def piece(at):
        here = pl.ds(at, ROWS)
        i = at // ROWS
        return (pltpu.make_async_copy(x_ref.at[here, :], x_s.at[i % 2], x_sems.at[i]),
                pltpu.make_async_copy(cs_ref.at[here, :], cs_s.at[i % 2], cs_sems.at[i]))

    @pl.when(n == 0)
    def _():
        for copy in [*piece(0), weight(0, wq_ref), *piece(ROWS)]:
            copy.start()

    for kind, ref in enumerate((wq_ref, wk_ref, wv_ref)):
        pl.when((n + 1 >= kind * per) & (n + 1 < (kind + 1) * per))(lambda ref=ref: weight(n + 1, ref).start())
    weight(n, wq_ref).wait()

    def prepare(at):
        for copy in piece(at):
            copy.wait()
        low = lax.broadcasted_iota(jnp.int32, (HEAD, HEAD), 1) < HEAD // 2
        gain = gain_ref[...].astype(jnp.float32).reshape(1, -1)
        for r in range(at, at + ROWS, HEAD):
            here = pl.ds(r, HEAD)
            mine = pl.ds(r - at, HEAD)
            wide = x_s[at // ROWS % 2, mine, :].astype(jnp.float32)
            scale = lax.rsqrt(jnp.mean(wide * wide, -1, keepdims=True) + 1e-6)
            normed = (wide * scale * gain).astype(jnp.bfloat16)
            for d in range(some_s.shape[0]):
                some_s[d, here, :] = normed[:, d * HEAD : (d + 1) * HEAD]
            cs = cs_s[at // ROWS % 2, mine, :]
            other = pltpu.roll(cs, HEAD // 2, 1)
            cos_s[here, :] = jnp.where(low, cs, other)
            sin_s[here, :] = jnp.where(low, -other, cs)
        if at + 2 * ROWS < rows:
            for copy in piece(at + 2 * ROWS):
                copy.start()

    def turned(t, here):
        t = t.astype(jnp.bfloat16).astype(jnp.float32)
        return (t * cos_s[here, :] + pltpu.roll(t, HEAD // 2, 1) * sin_s[here, :]).astype(jnp.bfloat16)

    def multiply(finish, first=False):
        before = None
        if first:
            prepare(0)
        for at in [*range(0, rows, ROWS), None]:
            t = None
            if at is not None:
                if first and at + ROWS < rows:
                    prepare(at + ROWS)
                t = dot(jnp.concatenate([some_s[d, at : at + ROWS, :] for d in range(some_s.shape[0])], 1), w_s[slot])
            if before is not None:
                start, done = before
                for r in range(0, ROWS, HEAD):
                    for h in range(step):
                        finish(done[r : r + HEAD, h * HEAD : (h + 1) * HEAD], start + r, h)
            before = at, t

    def query(t, at, h):
        q_s[at // HEAD, n * step + h] = turned(t, pl.ds(at, HEAD)).T

    def key(t, at, h):
        k_s[(n - per) * step + h, at : at + HEAD, :] = turned(t, pl.ds(at, HEAD))

    def value(t, at, h):
        v_s[at // HEAD, (n - 2 * per) * step + h] = t.astype(jnp.bfloat16).T

    pl.when(n == 0)(lambda: multiply(query, first=True))
    pl.when((n > 0) & (n < per))(lambda: multiply(query))
    pl.when((n >= per) & (n < 2 * per))(lambda: multiply(key))
    pl.when(n >= 2 * per)(lambda: multiply(value))


def kernel(n, flat_x_ref, gain_ref, cs_ref, wq_ref, wk_ref, wv_ref, wo_ref, x_ref, y_s, q_s, k_s, v_s, wo_s, sa, sb, seen_a, seen_b, sum_s, x_s,
           give_s, take_s, far_out, far_in, near_out, near_in, stage_s, cs_s, w_s, some_s, cos_s, sin_s,
           stage_sems, cs_sems, w_sems, wo_sems, x_sems, send_sems, recv_sems):
    heads, rows, _ = k_s.shape
    blocks = rows // BQ
    per = BQ // HEAD
    e = HEAD**-0.5 * LOG2E
    scores = (sa, sb)
    seens = (seen_a, seen_b)
    chips = n // 2
    me = lax.axis_index("tp")
    core, chip = lax.rem(me, 2), lax.div(me, 2)
    after, before, across = (lax.rem(chip + d, chips) for d in (1, chips - 1, 2))
    right, left, partner = 2 * after + core, 2 * before + core, 2 * chip + 1 - core
    part = BQ // n
    early, late = pl.ds(0, part // 2), pl.ds(part // 2, part // 2)

    def fetch_x(i):
        return pltpu.make_async_copy(x_ref.at[i, core, chip], x_s.at[i], x_sems.at[i])

    get_wo = [pltpu.make_async_copy(wo_ref.at[:, pl.ds(c * HEAD, HEAD)], wo_s.at[c], wo_sems.at[c]) for c in range(wo_s.shape[0])]
    barrier = pltpu.get_barrier_semaphore()
    for other in (left, right, partner):
        pl.semaphore_signal(barrier, inc=1, device_id={"tp": other}, device_id_type=pl.DeviceIdType.MESH)

    def project(i, _):
        project_step(i, flat_x_ref, gain_ref, cs_ref, wq_ref, wk_ref, wv_ref, q_s, k_s, v_s, stage_s, cs_s, w_s, some_s, cos_s, sin_s,
                     stage_sems, cs_sems, w_sems)

        @pl.when(i == 1)
        def _():
            for copy in [*get_wo, *map(fetch_x, range(blocks))]:
                copy.start()

    lax.fori_loop(0, 3 * wq_ref.shape[1] // COLS, project, None)
    pl.semaphore_wait(barrier, 3)

    def remote(c, kind, src, dst, to):
        return pltpu.make_async_remote_copy(src, dst, send_sems.at[c, kind], recv_sems.at[c, kind], device_id={"tp": to},
                                            device_id_type=pl.DeviceIdType.MESH)

    def copies(c):
        mine, other = y_s.at[c, core], y_s.at[c, core]
        return {
            0: (give_s.at[c], take_s.at[c], partner),
            1: (far_out.at[c, 0], far_in.at[c, 0], right),
            2: (far_out.at[c, 1], far_in.at[c, 1], left),
            3: (near_out.at[c, 0], near_in.at[c, 0], right),
            4: (near_out.at[c, 1], near_in.at[c, 1], left),
            5: (mine.at[chip], other.at[chip], right),
            6: (mine.at[chip], other.at[chip], left),
            7: (mine.at[chip], other.at[chip], partner),
            8: (mine.at[before, early], other.at[before, early], right),
            9: (mine.at[after, late], other.at[after, late], left),
            10: (mine.at[before], other.at[before], partner),
            11: (mine.at[after], other.at[after], partner),
            12: (mine.at[across], other.at[across], partner),
        }

    def start(c, *kinds):
        for kind in kinds:
            remote(c, kind, *copies(c)[kind]).start()

    def arrived(c, *kinds):
        for kind in kinds:
            remote(c, kind, *copies(c)[kind]).wait_recv()

    f32, bf16 = jnp.float32, jnp.bfloat16

    def stage(c, s):
        if s == 0:
            start(c, 0)
        if s == 1:
            arrived(c, 0)
            for q in range(chips):
                sum_s[c, q] = sum_s[c, q] + take_s[c, q].astype(f32)
            far_out[c, 0] = sum_s[c, across, early, :].astype(bf16)
            far_out[c, 1] = sum_s[c, across, late, :].astype(bf16)
            start(c, 1, 2)
        if s == 2:
            arrived(c, 1, 2)
            near_out[c, 0, early, :] = (sum_s[c, after, early, :] + far_in[c, 0].astype(f32)).astype(bf16)
            near_out[c, 0, late, :] = sum_s[c, after, late, :].astype(bf16)
            near_out[c, 1, early, :] = sum_s[c, before, early, :].astype(bf16)
            near_out[c, 1, late, :] = (sum_s[c, before, late, :] + far_in[c, 1].astype(f32)).astype(bf16)
            start(c, 3, 4)
        if s == 3:
            arrived(c, 3, 4)
            fetch_x(c).wait()
            total = sum_s[c, chip] + near_in[c, 0].astype(f32) + near_in[c, 1].astype(f32)
            y_s[c, core, chip] = (x_s[c].astype(f32) + total).astype(bf16)
            start(c, 5, 6, 7)
        if s == 4:
            arrived(c, 5, 6, 7)
            start(c, 8, 9, 10, 11)
        if s == 5:
            arrived(c, 8, 9, 10, 11)
            start(c, 12)
        if s == 6:
            arrived(c, 12)

    last_stage = 6
    flight = []

    clock = [0.0]

    def due(spent=None):
        clock[0] += spent or 0
        now = [(c, s) for c, s, ready in flight if spent is None or ready <= clock[0]]
        flight[:] = [(c, s + 1, clock[0] + TRAVEL[s]) if (c, s) in now else (c, s, ready) for c, s, ready in flight if (c, s) not in now or s < last_stage]
        return now

    def run(now):
        for c, s in now:
            stage(c, s)

    ones = jnp.ones((16, BQ), bf16)
    half = BQ // 2
    my_rows, other_rows = pl.multiple_of(core * half, half), pl.multiple_of((1 - core) * half, half)

    def output(c, at, tiles):
        weights = jnp.concatenate([wo_s[at + i] for i in range(tiles)], 1)
        term = dot(jnp.concatenate([seens[c % 2][h] for h in range(heads)], 1), weights)
        columns = pl.ds(pl.multiple_of(at * HEAD, HEAD), tiles * HEAD)
        for q in range(chips):
            sum_s[c, q, :, columns] = term[q * part : (q + 1) * part]
            give_s[c, q, :, columns] = term[half + q * part : half + (q + 1) * part].astype(bf16)

    out_tiles = wo_s.shape[0]
    for iq in range(blocks):
        tiles = iq + 1
        unroll = max(4, min(heads, 16 // tiles))
        unroll = max(u for u in (16, 8, 4, 2) if u <= unroll and heads % u == 0)

        def first(h, s_ref, j):
            tile = pl.ds(j * BQ, BQ)
            s = dot(k_s[h, tile, :], jnp.concatenate([q_s[iq * per + i, h] for i in range(per)], 1))
            if j == iq:
                seen = lax.broadcasted_iota(jnp.int32, (BQ, BQ), 0) <= lax.broadcasted_iota(jnp.int32, (BQ, BQ), 1)
                s = jnp.where(seen, s, HIDDEN)
            s_ref[tile, :] = s
            return s.reshape(BQ // 8, 8, BQ).max(0)

        def second(h, s_ref, j, top):
            tile = pl.ds(j * BQ, BQ)
            p = jnp.exp2((s_ref[tile, :] - top) * e).astype(bf16)
            values = jnp.concatenate([v_s[j * per + i, h] for i in range(per)], 1)
            return dot(jnp.concatenate([values, ones], 0), p)

        def peak(parts):
            m = parts[0]
            for part in parts[1:]:
                m = jnp.maximum(m, part)
            return m.max(axis=0, keepdims=True)

        def finish(h, total):
            seen_s = seens[iq % 2]
            done = (total[:HEAD] * (1 / total[HEAD : HEAD + 1])).astype(bf16).T
            seen_s[h, pl.ds(my_rows, half), :] = done[:half]
            seen_s[h, pl.ds(other_rows, half), :] = done[half:]

        plan = [due(unroll * (0.22 + 0.06 * tiles) + (0.9 * unroll / heads if 0 < iq < blocks - 1 else 0)) for _ in range(heads // unroll)]

        late_output = 0 < iq < blocks - 1
        groups = heads // unroll

        def group(g, top):
            for u in range(unroll):
                if late_output and u == unroll // 2:
                    output(iq - 1, g * (out_tiles // groups), out_tiles // groups)
                h = g * unroll + u
                later = jnp.minimum(h + 1, heads - 1)
                parts, total = [], None
                for j in range(tiles):
                    parts.append(first(later, scores[(u + 1) % 2], j))
                    got = second(h, scores[u % 2], j, top)
                    total = got if total is None else total + got
                finish(h, total)
                top = peak(parts)
            for i, now in enumerate(plan):
                if now:
                    pl.when(g == i)(functools.partial(run, now))
            return top

        top = peak([first(0, scores[0], j) for j in range(tiles)])
        lax.fori_loop(0, heads // unroll, group, top)
        if iq == 0:
            for copy in get_wo:
                copy.wait()
        if late_output:
            flight.append((iq - 1, 0, clock[0]))
        if iq >= blocks - 2:
            output(iq, 0, out_tiles)
            clock[0] += 1.2
            flight.append((iq, 0, clock[0]))
        run(due(0))

    while flight:
        run(due())
    for c in range(blocks):
        for kind, copy in copies(c).items():
            remote(c, kind, *copy).wait_send()


def solve(n, x, gain, wq, wk, wv, wo):
    rows, wide = x.shape
    columns = wo.shape[0]
    heads = columns // HEAD
    any_ = pl.BlockSpec(memory_space=pl.ANY)
    bf16, f32 = jnp.bfloat16, jnp.float32
    blocks, chips, part = rows // BQ, n // 2, BQ // n
    cut = (blocks, 2, chips, part, wide)
    kinds = 13
    tiles = (rows // HEAD, heads, HEAD, HEAD)
    y = pl.pallas_call(
        functools.partial(kernel, n),
        in_specs=[any_, pl.BlockSpec(memory_space=pltpu.VMEM), *[any_] * 6],
        out_specs=pl.BlockSpec(memory_space=pltpu.VMEM),
        out_shape=pltpu.VMEM(cut, bf16),
        scratch_shapes=[
            pltpu.VMEM(tiles, bf16),
            pltpu.VMEM((heads, rows, HEAD), bf16),
            pltpu.VMEM(tiles, bf16),
            pltpu.VMEM((wide // HEAD, columns, HEAD), bf16),
            pltpu.VMEM((rows, BQ), f32),
            pltpu.VMEM((rows, BQ), f32),
            pltpu.VMEM((heads, BQ, HEAD), bf16),
            pltpu.VMEM((heads, BQ, HEAD), bf16),
            pltpu.VMEM((blocks, chips, part, wide), f32),
            pltpu.VMEM((blocks, part, wide), bf16),
            pltpu.VMEM((blocks, chips, part, wide), bf16),
            pltpu.VMEM((blocks, chips, part, wide), bf16),
            pltpu.VMEM((blocks, 2, part // 2, wide), bf16),
            pltpu.VMEM((blocks, 2, part // 2, wide), bf16),
            pltpu.VMEM((blocks, 2, part, wide), bf16),
            pltpu.VMEM((blocks, 2, part, wide), bf16),
            pltpu.VMEM((2, ROWS, wide), bf16),
            pltpu.VMEM((2, ROWS, HEAD), f32),
            pltpu.VMEM((2, wide, COLS), bf16),
            pltpu.VMEM((wide // HEAD, rows, HEAD), bf16),
            pltpu.VMEM((rows, HEAD), f32),
            pltpu.VMEM((rows, HEAD), f32),
            pltpu.SemaphoreType.DMA((rows // ROWS,)),
            pltpu.SemaphoreType.DMA((rows // ROWS,)),
            pltpu.SemaphoreType.DMA((2,)),
            pltpu.SemaphoreType.DMA((wide // HEAD,)),
            pltpu.SemaphoreType.DMA((blocks,)),
            pltpu.SemaphoreType.DMA((blocks, kinds)),
            pltpu.SemaphoreType.DMA((blocks, kinds)),
        ],
        compiler_params=pltpu.CompilerParams(vmem_limit_bytes=VMEM - 2 * 2**20, collective_id=0, has_side_effects=True),
        cost_estimate=pl.CostEstimate(flops=2 * rows * rows * columns + 8 * rows * wide * columns, transcendentals=rows * rows * heads // 2, bytes_accessed=8 * wide * columns),
    )(x, gain, jnp.asarray(table(rows)), wq, wk, wv, wo, x.reshape(cut))
    return y.reshape(rows, wide)


def solution(mesh):
    n = mesh.shape["tp"]

    def step(x, gain, wq, wk, wv, wo):
        return solve(n, x, gain, wq, wk, wv, wo)

    tokens, columns = P("dp", None), P(None, "tp")
    return jax.shard_map(
        step,
        mesh=mesh,
        in_specs=(tokens, P(None), columns, columns, columns, P("tp", None)),
        out_specs=tokens,
        check_vma=False,
    )
```

```python
import functools

import jax
import jax.numpy as jnp
import numpy as np
from jax import lax
from jax.experimental import pallas as pl
from jax.experimental.pallas import tpu as pltpu
from jax.sharding import PartitionSpec as P

HEAD = 128
THETA = 10000
HIDDEN = -2e30
LOG2E = 1.4426950408889634
VMEM = 60 * 2**20
COLS = 512
ROWS = 256
BQ = 256
TRAVEL = (2.2, 3.8, 4.6, 4.6, 3.8, 2.2, 0)


def dot(a, b):
    return lax.dot_general(a, b, (((1,), (0,)), ((), ())), preferred_element_type=jnp.float32)


def table(rows):
    half = HEAD // 2
    angle = np.arange(rows, dtype=np.float32)[:, None] * (np.float32(THETA) ** (-np.arange(half, dtype=np.float32) / half)).astype(np.float32)
    return np.concatenate([np.cos(angle.astype(np.float64)), np.sin(angle.astype(np.float64))], -1).astype(np.float32)


def project_step(n, x_ref, gain_ref, cs_ref, wq_ref, wk_ref, wv_ref, q_s, k_s, v_s, x_s, cs_s, w_s, some_s, cos_s, sin_s, x_sems, cs_sems, w_sems):
    rows = some_s.shape[1]
    per = wq_ref.shape[1] // COLS
    slot = lax.rem(n, 2)
    step = COLS // HEAD

    def weight(i, ref):
        return pltpu.make_async_copy(ref.at[:, pl.ds(pl.multiple_of(lax.rem(i, per) * COLS, COLS), COLS)], w_s.at[lax.rem(i, 2)], w_sems.at[lax.rem(i, 2)])

    def piece(at):
        here = pl.ds(at, ROWS)
        i = at // ROWS
        return (pltpu.make_async_copy(x_ref.at[here, :], x_s.at[i % 2], x_sems.at[i]),
                pltpu.make_async_copy(cs_ref.at[here, :], cs_s.at[i % 2], cs_sems.at[i]))

    @pl.when(n == 0)
    def _():
        for copy in [*piece(0), weight(0, wq_ref), *piece(ROWS)]:
            copy.start()

    for kind, ref in enumerate((wq_ref, wk_ref, wv_ref)):
        pl.when((n + 1 >= kind * per) & (n + 1 < (kind + 1) * per))(lambda ref=ref: weight(n + 1, ref).start())
    weight(n, wq_ref).wait()

    def prepare(at):
        for copy in piece(at):
            copy.wait()
        low = lax.broadcasted_iota(jnp.int32, (HEAD, HEAD), 1) < HEAD // 2
        gain = gain_ref[...].astype(jnp.float32).reshape(1, -1)
        for r in range(at, at + ROWS, HEAD):
            here = pl.ds(r, HEAD)
            mine = pl.ds(r - at, HEAD)
            wide = x_s[at // ROWS % 2, mine, :].astype(jnp.float32)
            scale = lax.rsqrt(jnp.mean(wide * wide, -1, keepdims=True) + 1e-6)
            normed = (wide * scale * gain).astype(jnp.bfloat16)
            for d in range(some_s.shape[0]):
                some_s[d, here, :] = normed[:, d * HEAD : (d + 1) * HEAD]
            cs = cs_s[at // ROWS % 2, mine, :]
            other = pltpu.roll(cs, HEAD // 2, 1)
            cos_s[here, :] = jnp.where(low, cs, other)
            sin_s[here, :] = jnp.where(low, -other, cs)
        if at + 2 * ROWS < rows:
            for copy in piece(at + 2 * ROWS):
                copy.start()

    def turned(t, here):
        t = t.astype(jnp.bfloat16).astype(jnp.float32)
        return (t * cos_s[here, :] + pltpu.roll(t, HEAD // 2, 1) * sin_s[here, :]).astype(jnp.bfloat16)

    def multiply(finish, first=False):
        before = None
        if first:
            prepare(0)
        for at in [*range(0, rows, ROWS), None]:
            t = None
            if at is not None:
                if first and at + ROWS < rows:
                    prepare(at + ROWS)
                t = dot(jnp.concatenate([some_s[d, at : at + ROWS, :] for d in range(some_s.shape[0])], 1), w_s[slot])
            if before is not None:
                start, done = before
                for r in range(0, ROWS, HEAD):
                    for h in range(step):
                        finish(done[r : r + HEAD, h * HEAD : (h + 1) * HEAD], start + r, h)
            before = at, t

    def query(t, at, h):
        q_s[at // HEAD, n * step + h] = turned(t, pl.ds(at, HEAD)).T

    def key(t, at, h):
        k_s[(n - per) * step + h, at : at + HEAD, :] = turned(t, pl.ds(at, HEAD))

    def value(t, at, h):
        v_s[at // HEAD, (n - 2 * per) * step + h] = t.astype(jnp.bfloat16).T

    pl.when(n == 0)(lambda: multiply(query, first=True))
    pl.when((n > 0) & (n < per))(lambda: multiply(query))
    pl.when((n >= per) & (n < 2 * per))(lambda: multiply(key))
    pl.when(n >= 2 * per)(lambda: multiply(value))


def kernel(n, flat_x_ref, gain_ref, cs_ref, wq_ref, wk_ref, wv_ref, wo_ref, x_ref, y_s, q_s, k_s, v_s, wo_s, sa, sb, seen_a, seen_b, sum_s, x_s,
           give_s, take_s, far_out, far_in, near_out, near_in, stage_s, cs_s, w_s, some_s, cos_s, sin_s,
           stage_sems, cs_sems, w_sems, wo_sems, x_sems, send_sems, recv_sems):
    heads, rows, _ = k_s.shape
    blocks = rows // BQ
    per = BQ // HEAD
    e = HEAD**-0.5 * LOG2E
    scores = (sa, sb)
    seens = (seen_a, seen_b)
    chips = n // 2
    me = lax.axis_index("tp")
    core, chip = lax.rem(me, 2), lax.div(me, 2)
    after, before, across = (lax.rem(chip + d, chips) for d in (1, chips - 1, 2))
    right, left, partner = 2 * after + core, 2 * before + core, 2 * chip + 1 - core
    part = BQ // n
    early, late = pl.ds(0, part // 2), pl.ds(part // 2, part // 2)

    def fetch_x(i):
        return pltpu.make_async_copy(x_ref.at[i, core, chip], x_s.at[i], x_sems.at[i])

    get_wo = [pltpu.make_async_copy(wo_ref.at[:, pl.ds(c * HEAD, HEAD)], wo_s.at[c], wo_sems.at[c]) for c in range(wo_s.shape[0])]
    barrier = pltpu.get_barrier_semaphore()
    for other in (left, right, partner):
        pl.semaphore_signal(barrier, inc=1, device_id={"tp": other}, device_id_type=pl.DeviceIdType.MESH)

    def project(i, _):
        project_step(i, flat_x_ref, gain_ref, cs_ref, wq_ref, wk_ref, wv_ref, q_s, k_s, v_s, stage_s, cs_s, w_s, some_s, cos_s, sin_s,
                     stage_sems, cs_sems, w_sems)

        @pl.when(i == 1)
        def _():
            for copy in [*get_wo, *map(fetch_x, range(blocks))]:
                copy.start()

    lax.fori_loop(0, 3 * wq_ref.shape[1] // COLS, project, None)
    pl.semaphore_wait(barrier, 3)

    def remote(c, kind, src, dst, to):
        return pltpu.make_async_remote_copy(src, dst, send_sems.at[c, kind], recv_sems.at[c, kind], device_id={"tp": to},
                                            device_id_type=pl.DeviceIdType.MESH)

    def copies(c):
        mine, other = y_s.at[c, core], y_s.at[c, core]
        return {
            0: (give_s.at[c], take_s.at[c], partner),
            1: (far_out.at[c, 0], far_in.at[c, 0], right),
            2: (far_out.at[c, 1], far_in.at[c, 1], left),
            3: (near_out.at[c, 0], near_in.at[c, 0], right),
            4: (near_out.at[c, 1], near_in.at[c, 1], left),
            5: (mine.at[chip], other.at[chip], right),
            6: (mine.at[chip], other.at[chip], left),
            7: (mine.at[chip], other.at[chip], partner),
            8: (mine.at[before, early], other.at[before, early], right),
            9: (mine.at[after, late], other.at[after, late], left),
            10: (mine.at[before], other.at[before], partner),
            11: (mine.at[after], other.at[after], partner),
            12: (mine.at[across], other.at[across], partner),
        }

    def start(c, *kinds):
        for kind in kinds:
            remote(c, kind, *copies(c)[kind]).start()

    def arrived(c, *kinds):
        for kind in kinds:
            remote(c, kind, *copies(c)[kind]).wait_recv()

    f32, bf16 = jnp.float32, jnp.bfloat16

    def stage(c, s):
        if s == 0:
            start(c, 0)
        if s == 1:
            arrived(c, 0)
            for q in range(chips):
                sum_s[c, q] = sum_s[c, q] + take_s[c, q].astype(f32)
            far_out[c, 0] = sum_s[c, across, early, :].astype(bf16)
            far_out[c, 1] = sum_s[c, across, late, :].astype(bf16)
            start(c, 1, 2)
        if s == 2:
            arrived(c, 1, 2)
            near_out[c, 0, early, :] = (sum_s[c, after, early, :] + far_in[c, 0].astype(f32)).astype(bf16)
            near_out[c, 0, late, :] = sum_s[c, after, late, :].astype(bf16)
            near_out[c, 1, early, :] = sum_s[c, before, early, :].astype(bf16)
            near_out[c, 1, late, :] = (sum_s[c, before, late, :] + far_in[c, 1].astype(f32)).astype(bf16)
            start(c, 3, 4)
        if s == 3:
            arrived(c, 3, 4)
            fetch_x(c).wait()
            total = sum_s[c, chip] + near_in[c, 0].astype(f32) + near_in[c, 1].astype(f32)
            y_s[c, core, chip] = (x_s[c].astype(f32) + total).astype(bf16)
            start(c, 5, 6, 7)
        if s == 4:
            arrived(c, 5, 6, 7)
            start(c, 8, 9, 10, 11)
        if s == 5:
            arrived(c, 8, 9, 10, 11)
            start(c, 12)
        if s == 6:
            arrived(c, 12)

    last_stage = 6
    flight = []

    clock = [0.0]

    def due(spent=None):
        clock[0] += spent or 0
        now = [(c, s) for c, s, ready in flight if spent is None or ready <= clock[0]]
        flight[:] = [(c, s + 1, clock[0] + TRAVEL[s]) if (c, s) in now else (c, s, ready) for c, s, ready in flight if (c, s) not in now or s < last_stage]
        return now

    def run(now):
        for c, s in now:
            stage(c, s)

    ones = jnp.ones((16, BQ), bf16)
    half = BQ // 2
    my_rows, other_rows = pl.multiple_of(core * half, half), pl.multiple_of((1 - core) * half, half)

    def output(c, at, tiles):
        weights = jnp.concatenate([wo_s[at + i] for i in range(tiles)], 1)
        term = dot(jnp.concatenate([seens[c % 2][h] for h in range(heads)], 1), weights)
        columns = pl.ds(pl.multiple_of(at * HEAD, HEAD), tiles * HEAD)
        for q in range(chips):
            sum_s[c, q, :, columns] = term[q * part : (q + 1) * part]
            give_s[c, q, :, columns] = term[half + q * part : half + (q + 1) * part].astype(bf16)

    out_tiles = wo_s.shape[0]
    for iq in range(blocks):
        tiles = iq + 1
        unroll = max(4, min(heads, 16 // tiles if tiles < 3 else 32 // tiles))
        unroll = max(u for u in (16, 8, 4, 2) if u <= unroll and heads % u == 0)

        def first(h, s_ref, j):
            tile = pl.ds(j * BQ, BQ)
            s = dot(k_s[h, tile, :], jnp.concatenate([q_s[iq * per + i, h] for i in range(per)], 1))
            if j == iq:
                seen = lax.broadcasted_iota(jnp.int32, (BQ, BQ), 0) <= lax.broadcasted_iota(jnp.int32, (BQ, BQ), 1)
                s = jnp.where(seen, s, HIDDEN)
            s_ref[tile, :] = s
            return s.reshape(BQ // 8, 8, BQ).max(0)

        def second(h, s_ref, j, top):
            tile = pl.ds(j * BQ, BQ)
            p = jnp.exp2((s_ref[tile, :] - top) * e).astype(bf16)
            values = jnp.concatenate([v_s[j * per + i, h] for i in range(per)], 1)
            return dot(jnp.concatenate([values, ones], 0), p)

        def peak(parts):
            m = parts[0]
            for part in parts[1:]:
                m = jnp.maximum(m, part)
            return m.max(axis=0, keepdims=True)

        def finish(h, total):
            seen_s = seens[iq % 2]
            done = (total[:HEAD] * (1 / total[HEAD : HEAD + 1])).astype(bf16).T
            seen_s[h, pl.ds(my_rows, half), :] = done[:half]
            seen_s[h, pl.ds(other_rows, half), :] = done[half:]

        plan = [due(unroll * (0.22 + 0.06 * tiles) + (0.9 * unroll / heads if 0 < iq < blocks - 1 else 0)) for _ in range(heads // unroll)]

        late_output = 0 < iq < blocks - 1
        groups = heads // unroll

        def group(g, top):
            for u in range(unroll):
                if late_output and u == unroll // 2:
                    output(iq - 1, g * (out_tiles // groups), out_tiles // groups)
                h = g * unroll + u
                later = jnp.minimum(h + 1, heads - 1)
                parts, total = [], None
                for j in range(tiles):
                    parts.append(first(later, scores[(u + 1) % 2], j))
                    got = second(h, scores[u % 2], j, top)
                    total = got if total is None else total + got
                finish(h, total)
                top = peak(parts)
            for i, now in enumerate(plan):
                if now:
                    pl.when(g == i)(functools.partial(run, now))
            return top

        top = peak([first(0, scores[0], j) for j in range(tiles)])
        lax.fori_loop(0, heads // unroll, group, top)
        if iq == 0:
            for copy in get_wo:
                copy.wait()
        if late_output:
            flight.append((iq - 1, 0, clock[0]))
        if iq >= blocks - 2:
            output(iq, 0, out_tiles)
            clock[0] += 1.2
            flight.append((iq, 0, clock[0]))
        run(due(0))

    waiting = list(range(blocks))
    while waiting:
        run(due())
        left_now = [c for c in waiting if c not in [f[0] for f in flight]]
        for c in left_now:
            for kind, copy in copies(c).items():
                remote(c, kind, *copy).wait_send()
            waiting.remove(c)


def solve(n, x, gain, wq, wk, wv, wo):
    rows, wide = x.shape
    columns = wo.shape[0]
    heads = columns // HEAD
    any_ = pl.BlockSpec(memory_space=pl.ANY)
    bf16, f32 = jnp.bfloat16, jnp.float32
    blocks, chips, part = rows // BQ, n // 2, BQ // n
    cut = (blocks, 2, chips, part, wide)
    kinds = 13
    tiles = (rows // HEAD, heads, HEAD, HEAD)
    y = pl.pallas_call(
        functools.partial(kernel, n),
        in_specs=[any_, pl.BlockSpec(memory_space=pltpu.VMEM), *[any_] * 6],
        out_specs=pl.BlockSpec(memory_space=pltpu.VMEM),
        out_shape=pltpu.VMEM(cut, bf16),
        scratch_shapes=[
            pltpu.VMEM(tiles, bf16),
            pltpu.VMEM((heads, rows, HEAD), bf16),
            pltpu.VMEM(tiles, bf16),
            pltpu.VMEM((wide // HEAD, columns, HEAD), bf16),
            pltpu.VMEM((rows, BQ), f32),
            pltpu.VMEM((rows, BQ), f32),
            pltpu.VMEM((heads, BQ, HEAD), bf16),
            pltpu.VMEM((heads, BQ, HEAD), bf16),
            pltpu.VMEM((blocks, chips, part, wide), f32),
            pltpu.VMEM((blocks, part, wide), bf16),
            pltpu.VMEM((blocks, chips, part, wide), bf16),
            pltpu.VMEM((blocks, chips, part, wide), bf16),
            pltpu.VMEM((blocks, 2, part // 2, wide), bf16),
            pltpu.VMEM((blocks, 2, part // 2, wide), bf16),
            pltpu.VMEM((blocks, 2, part, wide), bf16),
            pltpu.VMEM((blocks, 2, part, wide), bf16),
            pltpu.VMEM((2, ROWS, wide), bf16),
            pltpu.VMEM((2, ROWS, HEAD), f32),
            pltpu.VMEM((2, wide, COLS), bf16),
            pltpu.VMEM((wide // HEAD, rows, HEAD), bf16),
            pltpu.VMEM((rows, HEAD), f32),
            pltpu.VMEM((rows, HEAD), f32),
            pltpu.SemaphoreType.DMA((rows // ROWS,)),
            pltpu.SemaphoreType.DMA((rows // ROWS,)),
            pltpu.SemaphoreType.DMA((2,)),
            pltpu.SemaphoreType.DMA((wide // HEAD,)),
            pltpu.SemaphoreType.DMA((blocks,)),
            pltpu.SemaphoreType.DMA((blocks, kinds)),
            pltpu.SemaphoreType.DMA((blocks, kinds)),
        ],
        compiler_params=pltpu.CompilerParams(vmem_limit_bytes=VMEM - 2 * 2**20, collective_id=0, has_side_effects=True),
        cost_estimate=pl.CostEstimate(flops=2 * rows * rows * columns + 8 * rows * wide * columns, transcendentals=rows * rows * heads // 2, bytes_accessed=8 * wide * columns),
    )(x, gain, jnp.asarray(table(rows)), wq, wk, wv, wo, x.reshape(cut))
    return y.reshape(rows, wide)


def solution(mesh):
    n = mesh.shape["tp"]

    def step(x, gain, wq, wk, wv, wo):
        return solve(n, x, gain, wq, wk, wv, wo)

    tokens, columns = P("dp", None), P(None, "tp")
    return jax.shard_map(
        step,
        mesh=mesh,
        in_specs=(tokens, P(None), columns, columns, columns, P("tp", None)),
        out_specs=tokens,
        check_vma=False,
    )
```

```python
import functools

import jax
import jax.numpy as jnp
import numpy as np
from jax import lax
from jax.experimental import pallas as pl
from jax.experimental.pallas import tpu as pltpu
from jax.sharding import PartitionSpec as P

HEAD = 128
THETA = 10000
HIDDEN = -2e30
LOG2E = 1.4426950408889634
VMEM = 60 * 2**20
COLS = 512
ROWS = 256
BQ = 256
TRAVEL = (2.2, 3.8, 4.6, 4.6, 3.8, 2.2, 0)


def dot(a, b):
    return lax.dot_general(a, b, (((1,), (0,)), ((), ())), preferred_element_type=jnp.float32)


def table(rows):
    half = HEAD // 2
    angle = np.arange(rows, dtype=np.float32)[:, None] * (np.float32(THETA) ** (-np.arange(half, dtype=np.float32) / half)).astype(np.float32)
    return np.concatenate([np.cos(angle.astype(np.float64)), np.sin(angle.astype(np.float64))], -1).astype(np.float32)


def project_step(n, x_ref, gain_ref, cs_ref, wq_ref, wk_ref, wv_ref, q_s, k_s, v_s, x_s, cs_s, w_s, some_s, cos_s, sin_s, x_sems, cs_sems, w_sems):
    rows = some_s.shape[1]
    per = wq_ref.shape[1] // COLS
    slot = lax.rem(n, 2)
    step = COLS // HEAD

    def weight(i, ref):
        return pltpu.make_async_copy(ref.at[:, pl.ds(pl.multiple_of(lax.rem(i, per) * COLS, COLS), COLS)], w_s.at[lax.rem(i, 2)], w_sems.at[lax.rem(i, 2)])

    def piece(at):
        here = pl.ds(at, ROWS)
        i = at // ROWS
        return (pltpu.make_async_copy(x_ref.at[here, :], x_s.at[i % 2], x_sems.at[i]),
                pltpu.make_async_copy(cs_ref.at[here, :], cs_s.at[i % 2], cs_sems.at[i]))

    @pl.when(n == 0)
    def _():
        for copy in [*piece(0), weight(0, wq_ref), *piece(ROWS)]:
            copy.start()

    for kind, ref in enumerate((wq_ref, wk_ref, wv_ref)):
        pl.when((n + 1 >= kind * per) & (n + 1 < (kind + 1) * per))(lambda ref=ref: weight(n + 1, ref).start())
    weight(n, wq_ref).wait()

    def prepare(at):
        for copy in piece(at):
            copy.wait()
        low = lax.broadcasted_iota(jnp.int32, (HEAD, HEAD), 1) < HEAD // 2
        gain = gain_ref[...].astype(jnp.float32).reshape(1, -1)
        for r in range(at, at + ROWS, HEAD):
            here = pl.ds(r, HEAD)
            mine = pl.ds(r - at, HEAD)
            wide = x_s[at // ROWS % 2, mine, :].astype(jnp.float32)
            scale = lax.rsqrt(jnp.mean(wide * wide, -1, keepdims=True) + 1e-6)
            normed = (wide * scale * gain).astype(jnp.bfloat16)
            for d in range(some_s.shape[0]):
                some_s[d, here, :] = normed[:, d * HEAD : (d + 1) * HEAD]
            cs = cs_s[at // ROWS % 2, mine, :]
            other = pltpu.roll(cs, HEAD // 2, 1)
            cos_s[here, :] = jnp.where(low, cs, other)
            sin_s[here, :] = jnp.where(low, -other, cs)
        if at + 2 * ROWS < rows:
            for copy in piece(at + 2 * ROWS):
                copy.start()

    def turned(t, here):
        t = t.astype(jnp.bfloat16).astype(jnp.float32)
        return (t * cos_s[here, :] + pltpu.roll(t, HEAD // 2, 1) * sin_s[here, :]).astype(jnp.bfloat16)

    def multiply(finish, first=False):
        before = None
        if first:
            prepare(0)
        for at in [*range(0, rows, ROWS), None]:
            t = None
            if at is not None:
                if first and at + ROWS < rows:
                    prepare(at + ROWS)
                t = dot(jnp.concatenate([some_s[d, at : at + ROWS, :] for d in range(some_s.shape[0])], 1), w_s[slot])
            if before is not None:
                start, done = before
                for r in range(0, ROWS, HEAD):
                    for h in range(step):
                        finish(done[r : r + HEAD, h * HEAD : (h + 1) * HEAD], start + r, h)
            before = at, t

    def query(t, at, h):
        q_s[at // HEAD, n * step + h] = turned(t, pl.ds(at, HEAD)).T

    def key(t, at, h):
        k_s[(n - per) * step + h, at : at + HEAD, :] = turned(t, pl.ds(at, HEAD))

    def value(t, at, h):
        v_s[at // HEAD, (n - 2 * per) * step + h] = t.astype(jnp.bfloat16).T

    pl.when(n == 0)(lambda: multiply(query, first=True))
    pl.when((n > 0) & (n < per))(lambda: multiply(query))
    pl.when((n >= per) & (n < 2 * per))(lambda: multiply(key))
    pl.when(n >= 2 * per)(lambda: multiply(value))


def kernel(n, flat_x_ref, gain_ref, cs_ref, wq_ref, wk_ref, wv_ref, wo_ref, x_ref, y_s, q_s, k_s, v_s, wo_s, sa, sb, seen_a, seen_b, sum_s, x_s,
           give_s, take_s, far_out, far_in, near_out, near_in, stage_s, cs_s, w_s, some_s, cos_s, sin_s,
           stage_sems, cs_sems, w_sems, wo_sems, x_sems, send_sems, recv_sems):
    heads, rows, _ = k_s.shape
    blocks = rows // BQ
    per = BQ // HEAD
    e = HEAD**-0.5 * LOG2E
    scores = (sa, sb)
    seens = (seen_a, seen_b)
    chips = n // 2
    me = lax.axis_index("tp")
    core, chip = lax.rem(me, 2), lax.div(me, 2)
    after, before, across = (lax.rem(chip + d, chips) for d in (1, chips - 1, 2))
    right, left, partner = 2 * after + core, 2 * before + core, 2 * chip + 1 - core
    part = BQ // n
    early, late = pl.ds(0, part // 2), pl.ds(part // 2, part // 2)

    def fetch_x(i):
        return pltpu.make_async_copy(x_ref.at[i, core, chip], x_s.at[i], x_sems.at[i])

    get_wo = [pltpu.make_async_copy(wo_ref.at[:, pl.ds(c * HEAD, HEAD)], wo_s.at[c], wo_sems.at[c]) for c in range(wo_s.shape[0])]
    barrier = pltpu.get_barrier_semaphore()
    for other in (left, right, partner):
        pl.semaphore_signal(barrier, inc=1, device_id={"tp": other}, device_id_type=pl.DeviceIdType.MESH)

    def project(i, _):
        project_step(i, flat_x_ref, gain_ref, cs_ref, wq_ref, wk_ref, wv_ref, q_s, k_s, v_s, stage_s, cs_s, w_s, some_s, cos_s, sin_s,
                     stage_sems, cs_sems, w_sems)

        @pl.when(i == 1)
        def _():
            for copy in [*get_wo, *map(fetch_x, range(blocks))]:
                copy.start()

    lax.fori_loop(0, 3 * wq_ref.shape[1] // COLS, project, None)
    pl.semaphore_wait(barrier, 3)

    def remote(c, kind, src, dst, to):
        return pltpu.make_async_remote_copy(src, dst, send_sems.at[c, kind], recv_sems.at[c, kind], device_id={"tp": to},
                                            device_id_type=pl.DeviceIdType.MESH)

    def copies(c):
        mine, other = y_s.at[c, core], y_s.at[c, core]
        return {
            0: (give_s.at[c], take_s.at[c], partner),
            1: (far_out.at[c, 0], far_in.at[c, 0], right),
            2: (far_out.at[c, 1], far_in.at[c, 1], left),
            3: (near_out.at[c, 0], near_in.at[c, 0], right),
            4: (near_out.at[c, 1], near_in.at[c, 1], left),
            5: (mine.at[chip], other.at[chip], right),
            6: (mine.at[chip], other.at[chip], left),
            7: (mine.at[chip], other.at[chip], partner),
            8: (mine.at[before, early], other.at[before, early], right),
            9: (mine.at[after, late], other.at[after, late], left),
            10: (mine.at[before], other.at[before], partner),
            11: (mine.at[after], other.at[after], partner),
            12: (mine.at[across], other.at[across], partner),
        }

    def start(c, *kinds):
        for kind in kinds:
            remote(c, kind, *copies(c)[kind]).start()

    def arrived(c, *kinds):
        for kind in kinds:
            remote(c, kind, *copies(c)[kind]).wait_recv()

    f32, bf16 = jnp.float32, jnp.bfloat16

    def stage(c, s):
        if s == 0:
            start(c, 0)
        if s == 1:
            arrived(c, 0)
            for q in range(chips):
                sum_s[c, q] = sum_s[c, q] + take_s[c, q].astype(f32)
            far_out[c, 0] = sum_s[c, across, early, :].astype(bf16)
            far_out[c, 1] = sum_s[c, across, late, :].astype(bf16)
            start(c, 1, 2)
        if s == 2:
            arrived(c, 1, 2)
            near_out[c, 0, early, :] = (sum_s[c, after, early, :] + far_in[c, 0].astype(f32)).astype(bf16)
            near_out[c, 0, late, :] = sum_s[c, after, late, :].astype(bf16)
            near_out[c, 1, early, :] = sum_s[c, before, early, :].astype(bf16)
            near_out[c, 1, late, :] = (sum_s[c, before, late, :] + far_in[c, 1].astype(f32)).astype(bf16)
            start(c, 3, 4)
        if s == 3:
            arrived(c, 3, 4)
            fetch_x(c).wait()
            total = sum_s[c, chip] + near_in[c, 0].astype(f32) + near_in[c, 1].astype(f32)
            y_s[c, core, chip] = (x_s[c].astype(f32) + total).astype(bf16)
            start(c, 5, 6, 7)
        if s == 4:
            arrived(c, 5, 6, 7)
            start(c, 8, 9, 10, 11)
        if s == 5:
            arrived(c, 8, 9, 10, 11)
            start(c, 12)
        if s == 6:
            arrived(c, 12)

    last_stage = 6
    flight = []

    clock = [0.0]

    def due(spent=None):
        clock[0] += spent or 0
        now = [(c, s) for c, s, ready in flight if spent is None or ready <= clock[0]]
        flight[:] = [(c, s + 1, clock[0] + TRAVEL[s]) if (c, s) in now else (c, s, ready) for c, s, ready in flight if (c, s) not in now or s < last_stage]
        return now

    def run(now):
        for c, s in now:
            stage(c, s)

    half = BQ // 2
    my_rows, other_rows = pl.multiple_of(core * half, half), pl.multiple_of((1 - core) * half, half)

    def output(c, at, tiles):
        weights = jnp.concatenate([wo_s[at + i] for i in range(tiles)], 1)
        term = dot(jnp.concatenate([seens[c % 2][h] for h in range(heads)], 1), weights)
        columns = pl.ds(pl.multiple_of(at * HEAD, HEAD), tiles * HEAD)
        for q in range(chips):
            sum_s[c, q, :, columns] = term[q * part : (q + 1) * part]
            give_s[c, q, :, columns] = term[half + q * part : half + (q + 1) * part].astype(bf16)

    out_tiles = wo_s.shape[0]
    for iq in range(blocks):
        tiles = iq + 1
        unroll = max(4, min(heads, 16 // tiles if tiles < 3 else 32 // tiles))
        unroll = max(u for u in (16, 8, 4, 2) if u <= unroll and heads % u == 0)

        def first(h, s_ref, j, ahead=0):
            tile = pl.ds(j * BQ, BQ)
            s = dot(k_s[h, tile, :], jnp.concatenate([q_s[(iq + ahead) * per + i, h] for i in range(per)], 1))
            if j >= iq:
                seen = lax.broadcasted_iota(jnp.int32, (BQ, BQ), 0) - (iq + ahead - j) * BQ <= lax.broadcasted_iota(jnp.int32, (BQ, BQ), 1)
                s = jnp.where(seen, s, HIDDEN)
            s_ref[tile, :] = s
            return s.reshape(BQ // 8, 8, BQ).max(0)

        def second(h, s_ref, j, top):
            tile = pl.ds(j * BQ, BQ)
            p = jnp.exp2((s_ref[tile, :] - top) * e)
            values = jnp.concatenate([v_s[j * per + i, h] for i in range(per)], 1)
            return dot(values, p.astype(bf16)), p.reshape(BQ // 8, 8, BQ).sum(0)

        def peak(parts):
            m = parts[0]
            for part in parts[1:]:
                m = jnp.maximum(m, part)
            return m.max(axis=0, keepdims=True)

        def finish(h, total, weight):
            seen_s = seens[iq % 2]
            done = (total * (1 / weight.sum(axis=0, keepdims=True))).astype(bf16).T
            seen_s[h, pl.ds(my_rows, half), :] = done[:half]
            seen_s[h, pl.ds(other_rows, half), :] = done[half:]

        plan = [due(unroll * (0.22 + 0.06 * tiles) + (0.9 * unroll / heads if 0 < iq < blocks - 1 else 0)) for _ in range(heads // unroll)]

        late_output = 0 < iq < blocks - 1
        groups = heads // unroll

        def group(g, top):
            for u in range(unroll):
                if late_output and u == unroll // 2:
                    output(iq - 1, g * (out_tiles // groups), out_tiles // groups)
                h = g * unroll + u
                later, ahead = h + 1, 0
                if u == unroll - 1:
                    later = lax.rem(later, heads)
                    ahead = jnp.where(later == 0, 1 if iq + 1 < blocks else 0, 0)
                parts, total, weight = [], None, None
                for j in range(tiles):
                    parts.append(first(later, scores[(u + 1) % 2], j, ahead))
                    got, more = second(h, scores[u % 2], j, top)
                    total, weight = (got, more) if total is None else (total + got, weight + more)
                finish(h, total, weight)
                top = peak(parts)
            for i, now in enumerate(plan):
                if now:
                    pl.when(g == i)(functools.partial(run, now))
            return top

        if iq == 0:
            top = peak([first(0, scores[0], 0)])
        top = lax.fori_loop(0, heads // unroll, group, top)
        if iq + 1 < blocks:
            top = jnp.maximum(top, peak([first(0, scores[0], iq + 1, 1)]))
        if iq == 0:
            for copy in get_wo:
                copy.wait()
        if late_output:
            flight.append((iq - 1, 0, clock[0]))
        if iq >= blocks - 2:
            output(iq, 0, out_tiles)
            clock[0] += 1.2
            flight.append((iq, 0, clock[0]))
        run(due(0))

    waiting = list(range(blocks))
    while waiting:
        run(due())
        left_now = [c for c in waiting if c not in [f[0] for f in flight]]
        for c in left_now:
            for kind, copy in copies(c).items():
                remote(c, kind, *copy).wait_send()
            waiting.remove(c)


def solve(n, x, gain, wq, wk, wv, wo):
    rows, wide = x.shape
    columns = wo.shape[0]
    heads = columns // HEAD
    any_ = pl.BlockSpec(memory_space=pl.ANY)
    bf16, f32 = jnp.bfloat16, jnp.float32
    blocks, chips, part = rows // BQ, n // 2, BQ // n
    cut = (blocks, 2, chips, part, wide)
    kinds = 13
    tiles = (rows // HEAD, heads, HEAD, HEAD)
    y = pl.pallas_call(
        functools.partial(kernel, n),
        in_specs=[any_, pl.BlockSpec(memory_space=pltpu.VMEM), *[any_] * 6],
        out_specs=pl.BlockSpec(memory_space=pltpu.VMEM),
        out_shape=pltpu.VMEM(cut, bf16),
        scratch_shapes=[
            pltpu.VMEM(tiles, bf16),
            pltpu.VMEM((heads, rows, HEAD), bf16),
            pltpu.VMEM(tiles, bf16),
            pltpu.VMEM((wide // HEAD, columns, HEAD), bf16),
            pltpu.VMEM((rows, BQ), f32),
            pltpu.VMEM((rows, BQ), f32),
            pltpu.VMEM((heads, BQ, HEAD), bf16),
            pltpu.VMEM((heads, BQ, HEAD), bf16),
            pltpu.VMEM((blocks, chips, part, wide), f32),
            pltpu.VMEM((blocks, part, wide), bf16),
            pltpu.VMEM((blocks, chips, part, wide), bf16),
            pltpu.VMEM((blocks, chips, part, wide), bf16),
            pltpu.VMEM((blocks, 2, part // 2, wide), bf16),
            pltpu.VMEM((blocks, 2, part // 2, wide), bf16),
            pltpu.VMEM((blocks, 2, part, wide), bf16),
            pltpu.VMEM((blocks, 2, part, wide), bf16),
            pltpu.VMEM((2, ROWS, wide), bf16),
            pltpu.VMEM((2, ROWS, HEAD), f32),
            pltpu.VMEM((2, wide, COLS), bf16),
            pltpu.VMEM((wide // HEAD, rows, HEAD), bf16),
            pltpu.VMEM((rows, HEAD), f32),
            pltpu.VMEM((rows, HEAD), f32),
            pltpu.SemaphoreType.DMA((rows // ROWS,)),
            pltpu.SemaphoreType.DMA((rows // ROWS,)),
            pltpu.SemaphoreType.DMA((2,)),
            pltpu.SemaphoreType.DMA((wide // HEAD,)),
            pltpu.SemaphoreType.DMA((blocks,)),
            pltpu.SemaphoreType.DMA((blocks, kinds)),
            pltpu.SemaphoreType.DMA((blocks, kinds)),
        ],
        compiler_params=pltpu.CompilerParams(vmem_limit_bytes=VMEM - 2 * 2**20, collective_id=0, has_side_effects=True),
        cost_estimate=pl.CostEstimate(flops=2 * rows * rows * columns + 8 * rows * wide * columns, transcendentals=rows * rows * heads // 2, bytes_accessed=8 * wide * columns),
    )(x, gain, jnp.asarray(table(rows)), wq, wk, wv, wo, x.reshape(cut))
    return y.reshape(rows, wide)


def solution(mesh):
    n = mesh.shape["tp"]

    def step(x, gain, wq, wk, wv, wo):
        return solve(n, x, gain, wq, wk, wv, wo)

    tokens, columns = P("dp", None), P(None, "tp")
    return jax.shard_map(
        step,
        mesh=mesh,
        in_specs=(tokens, P(None), columns, columns, columns, P("tp", None)),
        out_specs=tokens,
        check_vma=False,
    )
```

```python
import functools

import jax
import jax.numpy as jnp
import numpy as np
from jax import lax
from jax.experimental import pallas as pl
from jax.experimental.pallas import tpu as pltpu
from jax.sharding import PartitionSpec as P

HEAD = 128
THETA = 10000
HIDDEN = -2e30
LOG2E = 1.4426950408889634
VMEM = 60 * 2**20
COLS = 512
ROWS = 256
BQ = 256
TRAVEL = (2.2, 3.8, 4.6, 4.6, 3.8, 2.2, 0)


def dot(a, b):
    return lax.dot_general(a, b, (((1,), (0,)), ((), ())), preferred_element_type=jnp.float32)


def table(rows):
    half = HEAD // 2
    angle = np.arange(rows, dtype=np.float32)[:, None] * (np.float32(THETA) ** (-np.arange(half, dtype=np.float32) / half)).astype(np.float32)
    return np.concatenate([np.cos(angle.astype(np.float64)), np.sin(angle.astype(np.float64))], -1).astype(np.float32)


def project_step(n, x_ref, gain_ref, cs_ref, wq_ref, wk_ref, wv_ref, q_s, k_s, v_s, x_s, cs_s, w_s, some_s, cos_s, sin_s, x_sems, cs_sems, w_sems):
    rows = some_s.shape[1]
    per = wq_ref.shape[1] // COLS
    slot = lax.rem(n, 2)
    step = COLS // HEAD

    def weight(i, ref):
        return pltpu.make_async_copy(ref.at[:, pl.ds(pl.multiple_of(lax.rem(i, per) * COLS, COLS), COLS)], w_s.at[lax.rem(i, 2)], w_sems.at[lax.rem(i, 2)])

    def piece(at):
        here = pl.ds(at, ROWS)
        i = at // ROWS
        return (pltpu.make_async_copy(x_ref.at[here, :], x_s.at[i % 2], x_sems.at[i]),
                pltpu.make_async_copy(cs_ref.at[here, :], cs_s.at[i % 2], cs_sems.at[i]))

    @pl.when(n == 0)
    def _():
        for copy in [*piece(0), weight(0, wq_ref), *piece(ROWS)]:
            copy.start()

    for kind, ref in enumerate((wq_ref, wk_ref, wv_ref)):
        pl.when((n + 1 >= kind * per) & (n + 1 < (kind + 1) * per))(lambda ref=ref: weight(n + 1, ref).start())
    weight(n, wq_ref).wait()

    def prepare(at):
        for copy in piece(at):
            copy.wait()
        low = lax.broadcasted_iota(jnp.int32, (HEAD, HEAD), 1) < HEAD // 2
        gain = gain_ref[...].astype(jnp.float32).reshape(1, -1)
        for r in range(at, at + ROWS, HEAD):
            here = pl.ds(r, HEAD)
            mine = pl.ds(r - at, HEAD)
            wide = x_s[at // ROWS % 2, mine, :].astype(jnp.float32)
            scale = lax.rsqrt(jnp.mean(wide * wide, -1, keepdims=True) + 1e-6)
            normed = (wide * scale * gain).astype(jnp.bfloat16)
            for d in range(some_s.shape[0]):
                some_s[d, here, :] = normed[:, d * HEAD : (d + 1) * HEAD]
            cs = cs_s[at // ROWS % 2, mine, :]
            other = pltpu.roll(cs, HEAD // 2, 1)
            cos_s[here, :] = jnp.where(low, cs, other)
            sin_s[here, :] = jnp.where(low, -other, cs)
        if at + 2 * ROWS < rows:
            for copy in piece(at + 2 * ROWS):
                copy.start()

    def turned(t, here):
        t = t.astype(jnp.bfloat16).astype(jnp.float32)
        return (t * cos_s[here, :] + pltpu.roll(t, HEAD // 2, 1) * sin_s[here, :]).astype(jnp.bfloat16)

    def multiply(finish, first=False):
        before = None
        if first:
            prepare(0)
        for at in [*range(0, rows, ROWS), None]:
            t = None
            if at is not None:
                if first and at + ROWS < rows:
                    prepare(at + ROWS)
                t = dot(jnp.concatenate([some_s[d, at : at + ROWS, :] for d in range(some_s.shape[0])], 1), w_s[slot])
            if before is not None:
                start, done = before
                for r in range(0, ROWS, HEAD):
                    for h in range(step):
                        finish(done[r : r + HEAD, h * HEAD : (h + 1) * HEAD], start + r, h)
            before = at, t

    def query(t, at, h):
        q_s[at // HEAD, n * step + h] = turned(t, pl.ds(at, HEAD)).T

    def key(t, at, h):
        k_s[(n - per) * step + h, at : at + HEAD, :] = turned(t, pl.ds(at, HEAD))

    def value(t, at, h):
        v_s[at // HEAD, (n - 2 * per) * step + h] = t.astype(jnp.bfloat16).T

    pl.when(n == 0)(lambda: multiply(query, first=True))
    pl.when((n > 0) & (n < per))(lambda: multiply(query))
    pl.when((n >= per) & (n < 2 * per))(lambda: multiply(key))
    pl.when(n >= 2 * per)(lambda: multiply(value))


def kernel(n, flat_x_ref, gain_ref, cs_ref, wq_ref, wk_ref, wv_ref, wo_ref, x_ref, y_s, q_s, k_s, v_s, wo_s, sa, sb, seen_a, seen_b, sum_s, x_s,
           give_s, take_s, far_out, far_in, near_out, near_in, stage_s, cs_s, w_s, some_s, cos_s, sin_s,
           stage_sems, cs_sems, w_sems, wo_sems, x_sems, send_sems, recv_sems):
    heads, rows, _ = k_s.shape
    blocks = rows // BQ
    per = BQ // HEAD
    e = HEAD**-0.5 * LOG2E
    scores = (sa, sb)
    seens = (seen_a, seen_b)
    chips = n // 2
    me = lax.axis_index("tp")
    core, chip = lax.rem(me, 2), lax.div(me, 2)
    after, before, across = (lax.rem(chip + d, chips) for d in (1, chips - 1, 2))
    right, left, partner = 2 * after + core, 2 * before + core, 2 * chip + 1 - core
    part = BQ // n
    early, late = pl.ds(0, part // 2), pl.ds(part // 2, part // 2)

    def fetch_x(i):
        return pltpu.make_async_copy(x_ref.at[i, core, chip], x_s.at[i], x_sems.at[i])

    get_wo = [pltpu.make_async_copy(wo_ref.at[:, pl.ds(c * HEAD, HEAD)], wo_s.at[c], wo_sems.at[c]) for c in range(wo_s.shape[0])]
    barrier = pltpu.get_barrier_semaphore()
    for other in (left, right, partner):
        pl.semaphore_signal(barrier, inc=1, device_id={"tp": other}, device_id_type=pl.DeviceIdType.MESH)

    def project(i, _):
        project_step(i, flat_x_ref, gain_ref, cs_ref, wq_ref, wk_ref, wv_ref, q_s, k_s, v_s, stage_s, cs_s, w_s, some_s, cos_s, sin_s,
                     stage_sems, cs_sems, w_sems)

        @pl.when(i == 1)
        def _():
            for copy in [*get_wo, *map(fetch_x, range(blocks))]:
                copy.start()

    lax.fori_loop(0, 3 * wq_ref.shape[1] // COLS, project, None)
    pl.semaphore_wait(barrier, 3)

    def remote(c, kind, src, dst, to):
        return pltpu.make_async_remote_copy(src, dst, send_sems.at[c, kind], recv_sems.at[c, kind], device_id={"tp": to},
                                            device_id_type=pl.DeviceIdType.MESH)

    def copies(c):
        mine, other = y_s.at[c, core], y_s.at[c, core]
        return {
            0: (give_s.at[c], take_s.at[c], partner),
            1: (far_out.at[c, 0], far_in.at[c, 0], right),
            2: (far_out.at[c, 1], far_in.at[c, 1], left),
            3: (near_out.at[c, 0], near_in.at[c, 0], right),
            4: (near_out.at[c, 1], near_in.at[c, 1], left),
            5: (mine.at[chip], other.at[chip], right),
            6: (mine.at[chip], other.at[chip], left),
            7: (mine.at[chip], other.at[chip], partner),
            8: (mine.at[before, early], other.at[before, early], right),
            9: (mine.at[after, late], other.at[after, late], left),
            10: (mine.at[before], other.at[before], partner),
            11: (mine.at[after], other.at[after], partner),
            12: (mine.at[across], other.at[across], partner),
        }

    def start(c, *kinds):
        for kind in kinds:
            remote(c, kind, *copies(c)[kind]).start()

    def arrived(c, *kinds):
        for kind in kinds:
            remote(c, kind, *copies(c)[kind]).wait_recv()

    f32, bf16 = jnp.float32, jnp.bfloat16

    def stage(c, s):
        if s == 0:
            start(c, 0)
        if s == 1:
            arrived(c, 0)
            for q in range(chips):
                sum_s[c, q] = sum_s[c, q] + take_s[c, q].astype(f32)
            far_out[c, 0] = sum_s[c, across, early, :].astype(bf16)
            far_out[c, 1] = sum_s[c, across, late, :].astype(bf16)
            start(c, 1, 2)
        if s == 2:
            arrived(c, 1, 2)
            near_out[c, 0, early, :] = (sum_s[c, after, early, :] + far_in[c, 0].astype(f32)).astype(bf16)
            near_out[c, 0, late, :] = sum_s[c, after, late, :].astype(bf16)
            near_out[c, 1, early, :] = sum_s[c, before, early, :].astype(bf16)
            near_out[c, 1, late, :] = (sum_s[c, before, late, :] + far_in[c, 1].astype(f32)).astype(bf16)
            start(c, 3, 4)
        if s == 3:
            arrived(c, 3, 4)
            fetch_x(c).wait()
            total = sum_s[c, chip] + near_in[c, 0].astype(f32) + near_in[c, 1].astype(f32)
            y_s[c, core, chip] = (x_s[c].astype(f32) + total).astype(bf16)
            start(c, 5, 6, 7)
        if s == 4:
            arrived(c, 5, 6, 7)
            start(c, 8, 9, 10, 11)
        if s == 5:
            arrived(c, 8, 9, 10, 11)
            start(c, 12)
        if s == 6:
            arrived(c, 12)

    last_stage = 6
    flight = []

    clock = [0.0]

    def due(spent=None):
        clock[0] += spent or 0
        now = [(c, s) for c, s, ready in flight if spent is None or ready <= clock[0]]
        flight[:] = [(c, s + 1, clock[0] + TRAVEL[s]) if (c, s) in now else (c, s, ready) for c, s, ready in flight if (c, s) not in now or s < last_stage]
        return now

    def run(now):
        for c, s in now:
            stage(c, s)

    half = BQ // 2
    my_rows, other_rows = pl.multiple_of(core * half, half), pl.multiple_of((1 - core) * half, half)

    def output(c, at, tiles):
        weights = jnp.concatenate([wo_s[at + i] for i in range(tiles)], 1)
        term = dot(jnp.concatenate([seens[c % 2][h] for h in range(heads)], 1), weights)
        columns = pl.ds(pl.multiple_of(at * HEAD, HEAD), tiles * HEAD)
        for q in range(chips):
            sum_s[c, q, :, columns] = term[q * part : (q + 1) * part]
            give_s[c, q, :, columns] = term[half + q * part : half + (q + 1) * part].astype(bf16)

    out_tiles = wo_s.shape[0]
    for iq in range(blocks):
        tiles = iq + 1
        unroll = max(4, min(heads, 16 // tiles if tiles < 3 else 40 // tiles))
        unroll = max(u for u in (16, 8, 4, 2) if u <= unroll and heads % u == 0)

        def first(h, s_ref, j, ahead=0):
            tile = pl.ds(j * BQ, BQ)
            s = dot(k_s[h, tile, :], jnp.concatenate([q_s[(iq + ahead) * per + i, h] for i in range(per)], 1))
            if j >= iq:
                seen = lax.broadcasted_iota(jnp.int32, (BQ, BQ), 0) - (iq + ahead - j) * BQ <= lax.broadcasted_iota(jnp.int32, (BQ, BQ), 1)
                s = jnp.where(seen, s, HIDDEN)
            s_ref[tile, :] = s
            return s.reshape(BQ // 8, 8, BQ).max(0)

        def second(h, s_ref, j, top):
            tile = pl.ds(j * BQ, BQ)
            p = jnp.exp2((s_ref[tile, :] - top) * e)
            values = jnp.concatenate([v_s[j * per + i, h] for i in range(per)], 1)
            return dot(values, p.astype(bf16)), p.reshape(BQ // 8, 8, BQ).sum(0)

        def peak(parts):
            m = parts[0]
            for part in parts[1:]:
                m = jnp.maximum(m, part)
            return m.max(axis=0, keepdims=True)

        def finish(h, total, weight):
            seen_s = seens[iq % 2]
            done = (total * (1 / weight.sum(axis=0, keepdims=True))).astype(bf16).T
            seen_s[h, pl.ds(my_rows, half), :] = done[:half]
            seen_s[h, pl.ds(other_rows, half), :] = done[half:]

        plan = [due(unroll * (0.22 + 0.06 * tiles) + (0.9 * unroll / heads if 0 < iq < blocks - 1 else 0)) for _ in range(heads // unroll)]

        late_output = 0 < iq < blocks - 1
        groups = heads // unroll

        def group(g, top):
            for u in range(unroll):
                if late_output and u == unroll // 2:
                    output(iq - 1, g * (out_tiles // groups), out_tiles // groups)
                h = g * unroll + u
                later, ahead = h + 1, 0
                if u == unroll - 1:
                    later = lax.rem(later, heads)
                    ahead = jnp.where(later == 0, 1 if iq + 1 < blocks else 0, 0)
                parts, total, weight = [], None, None
                for j in range(tiles):
                    parts.append(first(later, scores[(u + 1) % 2], j, ahead))
                    got, more = second(h, scores[u % 2], j, top)
                    total, weight = (got, more) if total is None else (total + got, weight + more)
                finish(h, total, weight)
                top = peak(parts)
            for i, now in enumerate(plan):
                if now:
                    pl.when(g == i)(functools.partial(run, now))
            return top

        if iq == 0:
            top = peak([first(0, scores[0], 0)])
        top = lax.fori_loop(0, heads // unroll, group, top)
        if iq + 1 < blocks:
            top = jnp.maximum(top, peak([first(0, scores[0], iq + 1, 1)]))
        if iq == 0:
            for copy in get_wo:
                copy.wait()
        if late_output:
            flight.append((iq - 1, 0, clock[0]))
        if iq >= blocks - 2:
            output(iq, 0, out_tiles)
            clock[0] += 1.2
            flight.append((iq, 0, clock[0]))
        run(due(0))

    waiting = list(range(blocks))
    while waiting:
        run(due())
        left_now = [c for c in waiting if c not in [f[0] for f in flight]]
        for c in left_now:
            for kind, copy in copies(c).items():
                remote(c, kind, *copy).wait_send()
            waiting.remove(c)


def solve(n, x, gain, wq, wk, wv, wo):
    rows, wide = x.shape
    columns = wo.shape[0]
    heads = columns // HEAD
    any_ = pl.BlockSpec(memory_space=pl.ANY)
    bf16, f32 = jnp.bfloat16, jnp.float32
    blocks, chips, part = rows // BQ, n // 2, BQ // n
    cut = (blocks, 2, chips, part, wide)
    kinds = 13
    tiles = (rows // HEAD, heads, HEAD, HEAD)
    y = pl.pallas_call(
        functools.partial(kernel, n),
        in_specs=[any_, pl.BlockSpec(memory_space=pltpu.VMEM), *[any_] * 6],
        out_specs=pl.BlockSpec(memory_space=pltpu.VMEM),
        out_shape=pltpu.VMEM(cut, bf16),
        scratch_shapes=[
            pltpu.VMEM(tiles, bf16),
            pltpu.VMEM((heads, rows, HEAD), bf16),
            pltpu.VMEM(tiles, bf16),
            pltpu.VMEM((wide // HEAD, columns, HEAD), bf16),
            pltpu.VMEM((rows, BQ), f32),
            pltpu.VMEM((rows, BQ), f32),
            pltpu.VMEM((heads, BQ, HEAD), bf16),
            pltpu.VMEM((heads, BQ, HEAD), bf16),
            pltpu.VMEM((blocks, chips, part, wide), f32),
            pltpu.VMEM((blocks, part, wide), bf16),
            pltpu.VMEM((blocks, chips, part, wide), bf16),
            pltpu.VMEM((blocks, chips, part, wide), bf16),
            pltpu.VMEM((blocks, 2, part // 2, wide), bf16),
            pltpu.VMEM((blocks, 2, part // 2, wide), bf16),
            pltpu.VMEM((blocks, 2, part, wide), bf16),
            pltpu.VMEM((blocks, 2, part, wide), bf16),
            pltpu.VMEM((2, ROWS, wide), bf16),
            pltpu.VMEM((2, ROWS, HEAD), f32),
            pltpu.VMEM((2, wide, COLS), bf16),
            pltpu.VMEM((wide // HEAD, rows, HEAD), bf16),
            pltpu.VMEM((rows, HEAD), f32),
            pltpu.VMEM((rows, HEAD), f32),
            pltpu.SemaphoreType.DMA((rows // ROWS,)),
            pltpu.SemaphoreType.DMA((rows // ROWS,)),
            pltpu.SemaphoreType.DMA((2,)),
            pltpu.SemaphoreType.DMA((wide // HEAD,)),
            pltpu.SemaphoreType.DMA((blocks,)),
            pltpu.SemaphoreType.DMA((blocks, kinds)),
            pltpu.SemaphoreType.DMA((blocks, kinds)),
        ],
        compiler_params=pltpu.CompilerParams(vmem_limit_bytes=VMEM - 2 * 2**20, collective_id=0, has_side_effects=True),
        cost_estimate=pl.CostEstimate(flops=2 * rows * rows * columns + 8 * rows * wide * columns, transcendentals=rows * rows * heads // 2, bytes_accessed=8 * wide * columns),
    )(x, gain, jnp.asarray(table(rows)), wq, wk, wv, wo, x.reshape(cut))
    return y.reshape(rows, wide)


def solution(mesh):
    n = mesh.shape["tp"]

    def step(x, gain, wq, wk, wv, wo):
        return solve(n, x, gain, wq, wk, wv, wo)

    tokens, columns = P("dp", None), P(None, "tp")
    return jax.shard_map(
        step,
        mesh=mesh,
        in_specs=(tokens, P(None), columns, columns, columns, P("tp", None)),
        out_specs=tokens,
        check_vma=False,
    )
```
